512 devices in a mesh: pb: 16 (over x, y_lo, core), dev: 32 (over z, y_hi).
Axes of the slice: x: 4, y: 4 (y_hi: 2, y_lo: 2; y = y_hi * 2 + y_lo), z: 16, core: 2. Of those that a mesh axis runs over, the one named last changes fastest.
Arguments:
- queries: bfloat16 [1024, 768], P(('pb', 'dev')), may hold values from -6 to 6
- probes: int32 [1024, 16], P(('pb', 'dev')), may hold values from 0 to 1023, all different within a row
- vectors: bfloat16 [262144, 768], P(('pb', 'dev')), may hold values from -0.4375 to 0.4375
- list_ids: int32 [262144], P(('pb', 'dev')), may hold values from 0 to 1023, as said below
Outputs:
- leaders: float32 [1024, 100], P(('pb', 'dev'))
The draws below stay inside these ranges and needn't reach their ends.
Inputs may be any that keep to these rules, and one draw needn't show every extreme that they name: `list_ids`: each list id names exactly 256 database vectors. `probes`: each query names 16 different lists.
All inputs are finite; a program needn't handle non-finite values.
Results may differ from the reference program's by a relative error of at most 0.0004.
Values may be sent and summed in bfloat16 or wider, within the bound.
A program may use at most 64 MiB of HBM per device.

```python
import math
import jax
import jax.numpy as jnp
from jax import lax

D = 768
K = 100
NLIST = 1024
NPROBE = 16
QUERIES = 1024
VECTORS = 262144


def draw_list_ids(key, part):
    order = jax.random.permutation(key, VECTORS)
    return (order % NLIST).astype(jnp.int32)


def block_levels(own_key, shape, pieces, least, largest):
    factor_of, own = 1.0, jax.random.fold_in(own_key, 6)
    for dim, shards_of in pieces:
        heights = jnp.exp(jax.random.uniform(jax.random.fold_in(own, dim), (shards_of,), jnp.float32, least / len(pieces), largest / len(pieces)))
        factor_of = factor_of * jnp.repeat(heights, shape[dim] // shards_of).reshape([-1 if axis == dim else 1 for axis in range(len(shape))])
    return factor_of


def choose_distinct(key, rows, amount, top, lift):
    ranking = jax.random.permutation(jax.random.fold_in(key, 1), amount)
    boost = ranking
    for power in range(3):
        boost = boost * boost // amount
    boost = boost * lift // amount
    tickets = jax.random.randint(jax.random.fold_in(key, 2), (rows, amount), 0, 4096) + boost
    fixed_rows = jax.random.permutation(jax.random.fold_in(key, 3), rows)[jnp.arange(amount) % rows]
    tickets = jnp.where(jnp.arange(rows)[:, None] == fixed_rows[None, :], 1 << 14, tickets)
    score = tickets * amount + jnp.arange(amount)
    return lax.top_k(score.astype(jnp.int32), top)[1].astype(jnp.int32)


def bell_draw(stream_key, shape, spread, bound, cuts=(), kind=jnp.bfloat16):
    drawn = spread * jax.random.normal(stream_key, shape, jnp.float32)
    if cuts:
        drawn = drawn * block_levels(stream_key, shape, cuts, -0.22, 0.18)
    return jnp.clip(drawn, -bound, bound).astype(kind)


def setup_inputs(seed: int = 0) -> dict:
    arg_keys = jax.random.split(jax.random.key(seed), 5)
    return {
        "queries": bell_draw(arg_keys[0], (QUERIES, D), 1.0, 6.0, ((0, 512),)),
        "probes": choose_distinct(arg_keys[1], QUERIES, NLIST, NPROBE, 128),
        "vectors": bell_draw(arg_keys[2], (VECTORS, D), (D // 4) ** -0.5, 0.4375, ((0, 512),)),
        "list_ids": draw_list_ids(jax.random.fold_in(arg_keys[4], 71), 0),
    }


def reference(queries, probes, vectors, list_ids):
    qblock = math.gcd(QUERIES, 256)
    vblock = math.gcd(VECTORS, 8192)
    slab_rows = vectors.reshape(VECTORS // vblock, vblock, D)
    slab_lists = list_ids.reshape(VECTORS // vblock, vblock)

    def search_block(block_args):
        block_rows, block_probes = block_args
        initial = jnp.full((qblock, K), -1.0e30, jnp.float32)

        def absorb(running, slab):
            slab_part, slab_ids = slab
            products = lax.dot_general(block_rows, slab_part, (((1,), (1,)), ((), ())), preferred_element_type=jnp.float32)
            probed = jnp.any(block_probes[:, :, None] == slab_ids[None, None, :], axis=1)
            filtered = jnp.where(probed, products, jnp.float32(-1.0e30))
            kept, _ = lax.top_k(jnp.concatenate([running, filtered], axis=1), K)
            return kept, None

        kept, _ = lax.scan(absorb, initial, (slab_rows, slab_lists))
        return kept

    leaders = lax.map(search_block, (queries.reshape(QUERIES // qblock, qblock, D), probes.reshape(QUERIES // qblock, qblock, NPROBE)))
    return leaders.reshape(QUERIES, K)
```

```python
import functools

import jax
import jax.numpy as jnp
from jax import lax
from jax.experimental import pallas as pl
from jax.experimental.pallas import tpu as pltpu
from jax.sharding import PartitionSpec as P

K = 100
SENT = 104
NEG = -1.0e30
MESH = pl.DeviceIdType.MESH
F32 = jnp.float32


def exchange(a, b):
    return jnp.maximum(a, b), jnp.minimum(a, b)


def sort_desc(xs):
    xs, n, p = list(xs), len(xs), 1
    while p < n:
        k = p
        while k >= 1:
            for j in range(k % p, n - k, 2 * k):
                for i in range(min(k, n - j - k)):
                    if (i + j) // (2 * p) == (i + j + k) // (2 * p):
                        xs[i + j], xs[i + j + k] = exchange(xs[i + j], xs[i + j + k])
            k //= 2
        p *= 2
    return xs


def clean_desc(xs):
    xs, d = list(xs), len(xs) // 2
    while d >= 1:
        for i in range(len(xs)):
            if i & d == 0:
                xs[i], xs[i + d] = exchange(xs[i], xs[i + d])
        d //= 2
    return xs


def merge_top(load_a, load_b, tmp_load, tmp_store, store):
    @pl.loop(0, 8)
    def _(g):
        for u in range(4):
            i = g * 4 + u
            m = [jnp.maximum(load_a(i + 32 * k), load_b(127 - i - 32 * k)) for k in range(4)]
            m[0], m[2] = exchange(m[0], m[2])
            m[1], m[3] = exchange(m[1], m[3])
            m[0], m[1] = exchange(m[0], m[1])
            m[2], m[3] = exchange(m[2], m[3])
            for k in range(4):
                tmp_store(i + 32 * k, m[k])

    @pl.loop(0, 4)
    def _(k):
        xs = clean_desc([tmp_load(32 * k + i) for i in range(32)])
        for i in range(32):
            store(32 * k + i, xs[i])


def kernel(
    q_ref, p_ref, v_hbm, id_ref, o_ref,
    zbuf, gath, v_vm, prod, words, codes, runs, runs2, csend, crecv, ctmp,
    xsend, xrecv, atmp, apair, row_a, row_b, row_c, ysend, yrecv, zsend, zrecv,
    v_sem, zs, zr, fs, fr, ss, sr, cs, cr, rcs, rcr, rxs, rxr, rys, ryr, rzs, rzr,
):
    pb, dev = lax.axis_index("pb"), lax.axis_index("dev")
    x, ylo, c = pb // 4, (pb // 2) % 2, pb % 2
    z, yhi = dev // 2, dev % 2
    y = yhi * 2 + ylo

    def at(x_, y_, z_, c_):
        return {"pb": x_ * 4 + (y_ % 2) * 2 + c_, "dev": z_ * 2 + y_ // 2}

    z_peers = [at(x, y, (z + k) % 16, c) for k in range(1, 16)]
    y_peers = [at(x, (y + k) % 4, z, c) for k in range(1, 4)]
    x_peers = [at((x + k) % 4, y, z, c) for k in range(1, 4)]
    partner = at(x, y, z, 1 - c)

    barrier = pltpu.get_barrier_semaphore()
    everyone = z_peers + y_peers + x_peers + [partner]
    for peer in everyone:
        pl.semaphore_signal(barrier, inc=1, device_id=peer, device_id_type=MESH)

    v_copy = pltpu.make_async_copy(v_hbm, v_vm, v_sem)
    v_copy.start()

    zbuf[z, 12:16, :] = jnp.zeros((4, 128), jnp.bfloat16)
    for i in range(6):
        zbuf[z, 2 * i : 2 * i + 2, :] = q_ref[:, 128 * i : 128 * i + 128]
    lists = p_ref[...]
    zbuf[z, 12:14, 0:16] = (lists // 32).astype(F32).astype(jnp.bfloat16)
    zbuf[z, 12:14, 16:32] = (lists % 32).astype(F32).astype(jnp.bfloat16)
    for ref in (crecv, ):
        ref[...] = jnp.full(ref.shape, NEG, F32)
    for s in range(4):
        xrecv[s * 128 + SENT : s * 128 + 128, :] = jnp.full((128 - SENT, 128), NEG, F32)

    pl.semaphore_wait(barrier, len(everyone))

    def remote(src, dst, send, recv, peer):
        copy = pltpu.make_async_remote_copy(
            src_ref=src, dst_ref=dst, send_sem=send, recv_sem=recv,
            device_id=peer, device_id_type=MESH,
        )
        copy.start()
        return copy

    sent = []
    z_copies = [
        remote(zbuf.at[z], zbuf.at[z], zs.at[k], zr.at[k], z_peers[k]) for k in range(15)
    ]
    sent += z_copies
    r = lax.broadcasted_iota(jnp.int32, (224, 256), 0)
    k_ = lax.broadcasted_iota(jnp.int32, (224, 256), 1)
    pick = k_ == ((r % 32) // 2) * 16 + (r // 32) * 2 + r % 2
    pick = jnp.where(pick, 1.0, 0.0).astype(jnp.bfloat16)
    for copy in z_copies:
        copy.wait_recv()
    rows = jnp.dot(pick, zbuf[...].reshape(256, 128), preferred_element_type=F32)
    rows = rows.astype(jnp.bfloat16)
    for h in range(2):
        for i in range(7):
            gath[c, x, y, h, :, 128 * i : 128 * i + 128] = rows[
                32 * i + 16 * h : 32 * i + 16 * h + 16, :
            ]

    def piece(h, back1, back2):
        if h == 0:
            return gath.at[c, (x + 4 - back2) % 4, (y + 4 - back1) % 4, h]
        return gath.at[c, (x + 4 - back1) % 4, (y + 4 - back2) % 4, h]

    peers1 = [y_peers, x_peers]
    peers2 = [x_peers, y_peers]
    first, second, cross = {}, {}, {}
    for k in range(3):
        for h in range(2):
            ref = piece(h, 0, 0)
            first[h, k] = remote(ref, ref, fs.at[h, k], fr.at[h, k], peers1[h][k])

    def forward2(h, b):
        ref = piece(h, b, 0)
        for k in range(3):
            second[h, b, k] = remote(ref, ref, ss.at[h, b, k], sr.at[h, b, k], peers2[h][k])

    def forward_core(h, b1, b2):
        ref, n = piece(h, b1, b2), b1 * 4 + b2
        cross[h, b1, b2] = remote(ref, ref, cs.at[h, n], cr.at[h, n], partner)

    for h in range(2):
        forward2(h, 0)
    for h in range(2):
        forward_core(h, 0, 0)
    for b in (1, 3, 2):
        for h in range(2):
            first[h, b - 1].wait_recv()
            forward2(h, b)
            forward_core(h, b, 0)
    for b1 in (0, 1, 3, 2):
        for b2 in (1, 3, 2):
            for h in range(2):
                second[h, b1, b2 - 1].wait_recv()
                forward_core(h, b1, b2)
    sent += list(first.values()) + list(second.values()) + list(cross.values())
    for copy in cross.values():
        copy.wait_recv()
    v_copy.wait()

    for s in range(8):
        part = gath[s // 4, s % 4].reshape(128, 896)[:, 768:896]
        turned = part.astype(F32).T
        codes[32 * s : 32 * s + 32, :] = turned[:32, :].astype(jnp.int32)

    @pl.loop(0, 4)
    def _(s2):
        block = gath[s2 // 2, pl.ds((s2 % 2) * 2, 2)].reshape(256, 896)[:, :768]
        for m in range(4):
            scores = lax.dot_general(
                v_vm[128 * m : 128 * m + 128, :], block,
                (((1,), (1,)), ((), ())), preferred_element_type=F32,
            )
            for j in range(16):
                for t in range(2):
                    row = pl.multiple_of((16 * m + j) * 64 + (s2 * 2 + t) * 8, 8)
                    prod[pl.ds(row, 8), :] = scores[8 * j : 8 * j + 8, 128 * t : 128 * t + 128]

    high = [codes[pl.ds(p, 8, stride=32), :] for p in range(16)]
    bits = [jnp.left_shift(jnp.int32(1), codes[pl.ds(16 + p, 8, stride=32), :]) for p in range(16)]

    @pl.loop(0, 32)
    def _(a):
        word = jnp.zeros((8, 128), jnp.int32)
        for p in range(16):
            word = word | jnp.where(high[p] == a, bits[p], 0)
        words[a] = word

    @pl.loop(0, 16)
    def _(g):
        xs = []
        for i in range(32):
            value = prod[pl.ds(g * 256 + (i // 8) * 64 + i % 8, 8, stride=8), :]
            which = id_ref[g * 32 + i]
            word = words[which // 32]
            keep = (word & jnp.left_shift(jnp.int32(1), which % 32)) != 0
            xs.append(jnp.where(keep, value, NEG))
        xs = sort_desc(xs)
        for i in range(32):
            runs[g * 32 + i] = xs[i]

    @pl.loop(0, 8)
    def _(g):
        base = g * 64
        for side, op in ((0, jnp.maximum), (1, jnp.minimum)):
            xs = [op(runs[base + i], runs[base + 63 - i]) for i in range(32)]
            xs = clean_desc(xs)
            for i in range(32):
                runs2[base + 32 * side + i] = xs[i]

    @pl.loop(0, 4)
    def _(g):
        base = g * 128
        for i in range(32):
            a, b = runs2[base + i], runs2[base + 127 - i]
            a2, b2 = runs2[base + 32 + i], runs2[base + 95 - i]
            h1, l1 = exchange(a, b)
            h2, l2 = exchange(a2, b2)
            h1, h2 = exchange(h1, h2)
            l1, l2 = exchange(l1, l2)
            runs[base + i], runs[base + 32 + i] = h1, h2
            runs[base + 64 + i], runs[base + 96 + i] = l1, l2

    @pl.loop(0, 16)
    def _(g):
        xs = clean_desc([runs[g * 32 + i] for i in range(32)])
        for i in range(32):
            runs2[g * 32 + i] = xs[i]

    def run_store(ref, base):
        def put(i, value):
            ref[base + i] = value
        return put

    def run_load(ref, base):
        return lambda i: ref[base + i]

    for g in range(2):
        merge_top(
            run_load(runs2, 256 * g), run_load(runs2, 256 * g + 128),
            run_load(runs, 256 * g), run_store(runs, 256 * g), run_store(runs2, 256 * g),
        )

    def split_store(i, value):
        csend[0, i] = value[0:4, :]
        csend[1, i] = value[4:8, :]

    merge_top(run_load(runs2, 0), run_load(runs2, 256), run_load(runs, 0), run_store(runs, 0), split_store)

    copy = remote(
        csend.at[1 - c, pl.ds(0, SENT)], crecv.at[pl.ds(0, SENT)], rcs.at[0], rcr.at[0], partner
    )
    sent.append(copy)
    copy.wait_recv()

    def x_store(i, value):
        xsend[pl.ds(i, 4, stride=128), :] = value

    merge_top(lambda i: csend[c, i], run_load(crecv, 0), run_load(ctmp, 0), run_store(ctmp, 0), x_store)

    def x_rows(s):
        return pl.ds(pl.multiple_of(s * 128, 128), SENT)

    copies = [
        remote(
            xsend.at[x_rows((x + k + 1) % 4)], xrecv.at[x_rows(x)],
            rxs.at[k], rxr.at[k], x_peers[k],
        )
        for k in range(3)
    ]
    sent += copies
    xrecv[x_rows(x), :] = xsend[x_rows(x), :]
    for copy in copies:
        copy.wait_recv()

    def pair_store(i, value):
        apair[pl.ds(i, 2, stride=128), :] = value

    merge_top(
        lambda i: xrecv[pl.ds(i, 2, stride=128), :], lambda i: xrecv[pl.ds(256 + i, 2, stride=128), :],
        run_load(atmp, 0), run_store(atmp, 0), pair_store,
    )

    def row_load(ref, base=0):
        return lambda i: ref[pl.ds(base + i, 1), :]

    def row_store(ref):
        def put(i, value):
            ref[pl.ds(i, 1), :] = value
        return put

    merge_top(row_load(apair), row_load(apair, 128), row_load(row_c), row_store(row_c), row_store(row_a))

    def fold_lanes(distance):
        row_b[...] = pltpu.roll(row_a[...], 128 - distance, axis=1)
        merge_top(row_load(row_a), row_load(row_b), row_load(row_c), row_store(row_c), row_store(row_a))

    ysend[...] = row_a[...].T

    def y_rows(s):
        return pl.ds(pl.multiple_of(s * 32, 32), 32)

    copies = [
        remote(
            ysend.at[y_rows((y + k + 1) % 4)], yrecv.at[y_rows(y)],
            rys.at[k], ryr.at[k], y_peers[k],
        )
        for k in range(3)
    ]
    sent += copies
    yrecv[y_rows(y), :] = ysend[y_rows(y), :]
    for copy in copies:
        copy.wait_recv()
    row_a[...] = yrecv[...].T
    fold_lanes(64)
    fold_lanes(32)

    turned = row_a[...].T
    for s in range(16):
        zsend[s] = turned[2 * s : 2 * s + 2, :]
    copies = [
        remote(zsend.at[(z + k + 1) % 16], zrecv.at[z], rzs.at[k], rzr.at[k], z_peers[k])
        for k in range(15)
    ]
    sent += copies
    zrecv[z] = zsend[z]
    for copy in copies:
        copy.wait_recv()
    row_b[32:128, :] = jnp.full((96, 128), NEG, F32)
    for s in range(16):
        row_b[2 * s : 2 * s + 2, :] = zrecv[s]
    row_a[...] = row_b[...].T
    for distance in (16, 8, 4, 2):
        fold_lanes(distance)
    o_ref[...] = row_a[...].T[0:2, 0:K]

    for copy in sent:
        copy.wait_send()


def local(queries, probes, vectors, list_ids):
    vmem = pl.BlockSpec(memory_space=pltpu.VMEM)
    dma = pltpu.SemaphoreType.DMA
    return pl.pallas_call(
        kernel,
        out_shape=jax.ShapeDtypeStruct((2, K), F32),
        in_specs=[
            vmem, vmem, pl.BlockSpec(memory_space=pl.ANY), pl.BlockSpec(memory_space=pltpu.SMEM),
        ],
        out_specs=vmem,
        scratch_shapes=[
            pltpu.VMEM((16, 16, 128), jnp.bfloat16),
            pltpu.VMEM((2, 4, 4, 2, 16, 896), jnp.bfloat16),
            pltpu.VMEM((512, 768), jnp.bfloat16),
            pltpu.VMEM((4096, 128), F32),
            pltpu.VMEM((32, 8, 128), jnp.int32),
            pltpu.VMEM((256, 128), jnp.int32),
            pltpu.VMEM((512, 8, 128), F32),
            pltpu.VMEM((512, 8, 128), F32),
            pltpu.VMEM((2, 128, 4, 128), F32),
            pltpu.VMEM((128, 4, 128), F32),
            pltpu.VMEM((128, 4, 128), F32),
            pltpu.VMEM((512, 128), F32),
            pltpu.VMEM((512, 128), F32),
            pltpu.VMEM((128, 2, 128), F32),
            pltpu.VMEM((256, 128), F32),
            pltpu.VMEM((128, 128), F32),
            pltpu.VMEM((128, 128), F32),
            pltpu.VMEM((128, 128), F32),
            pltpu.VMEM((128, 128), F32),
            pltpu.VMEM((128, 128), F32),
            pltpu.VMEM((16, 2, 128), F32),
            pltpu.VMEM((16, 2, 128), F32),
            dma, dma((15,)), dma((15,)), dma((2, 3)), dma((2, 3)), dma((2, 4, 3)), dma((2, 4, 3)),
            dma((2, 16)), dma((2, 16)), dma((1,)), dma((1,)), dma((3,)), dma((3,)),
            dma((3,)), dma((3,)), dma((15,)), dma((15,)),
        ],
        compiler_params=pltpu.CompilerParams(collective_id=0, has_side_effects=True),
    )(queries, probes, vectors, list_ids)


def solution(mesh):
    return jax.shard_map(
        local,
        mesh=mesh,
        in_specs=(
            P(("pb", "dev"), None),
            P(("pb", "dev"), None),
            P(("pb", "dev"), None),
            P(("pb", "dev")),
        ),
        out_specs=P(("pb", "dev"), None),
        check_vma=False,
    )
```

```python
import functools

import jax
import jax.numpy as jnp
from jax import lax
from jax.experimental import pallas as pl
from jax.experimental.pallas import tpu as pltpu
from jax.sharding import PartitionSpec as P

K = 100
SENT = 104
NEG = -1.0e30
MESH = pl.DeviceIdType.MESH
F32 = jnp.float32


def exchange(a, b):
    return jnp.maximum(a, b), jnp.minimum(a, b)


def sort_desc(xs):
    xs, n, p = list(xs), len(xs), 1
    while p < n:
        k = p
        while k >= 1:
            for j in range(k % p, n - k, 2 * k):
                for i in range(min(k, n - j - k)):
                    if (i + j) // (2 * p) == (i + j + k) // (2 * p):
                        xs[i + j], xs[i + j + k] = exchange(xs[i + j], xs[i + j + k])
            k //= 2
        p *= 2
    return xs


def clean_desc(xs):
    xs, d = list(xs), len(xs) // 2
    while d >= 1:
        for i in range(len(xs)):
            if i & d == 0:
                xs[i], xs[i + d] = exchange(xs[i], xs[i + d])
        d //= 2
    return xs


def merge_top(load_a, load_b, tmp_load, tmp_store, store):
    @pl.loop(0, 8)
    def _(g):
        for u in range(4):
            i = g * 4 + u
            m = [jnp.maximum(load_a(i + 32 * k), load_b(127 - i - 32 * k)) for k in range(4)]
            m[0], m[2] = exchange(m[0], m[2])
            m[1], m[3] = exchange(m[1], m[3])
            m[0], m[1] = exchange(m[0], m[1])
            m[2], m[3] = exchange(m[2], m[3])
            for k in range(4):
                tmp_store(i + 32 * k, m[k])

    @pl.loop(0, 4)
    def _(k):
        xs = clean_desc([tmp_load(32 * k + i) for i in range(32)])
        for i in range(32):
            store(32 * k + i, xs[i])


def kernel(
    q_hbm, p_hbm, v_hbm, id_hbm, o_ref,
    q_ref, p_ref, id_ref, zbuf, gath, v_vm, prod, words, codes, runs, runs2, csend, crecv, ctmp,
    xsend, xrecv, atmp, apair, row_a, row_b, row_c, ysend, yrecv, zsend, zrecv,
    in_sem, zs, zr, fs, fr, ss, sr, cs, cr, rcs, rcr, rxs, rxr, rys, ryr, rzs, rzr,
):
    pb, dev = lax.axis_index("pb"), lax.axis_index("dev")
    x, ylo, c = pb // 4, (pb // 2) % 2, pb % 2
    z, yhi = dev // 2, dev % 2
    y = yhi * 2 + ylo

    def at(x_, y_, z_, c_):
        return {"pb": x_ * 4 + (y_ % 2) * 2 + c_, "dev": z_ * 2 + y_ // 2}

    z_peers = {k: at(x, y, (z + k) % 16, c) for k in range(1, 16)}
    y_peers = [at(x, (y + k) % 4, z, c) for k in range(1, 4)]
    x_peers = [at((x + k) % 4, y, z, c) for k in range(1, 4)]
    partner = at(x, y, z, 1 - c)

    barrier = pltpu.get_barrier_semaphore()
    near = (4, 12, 3, 13, 2, 14, 1, 15)
    everyone = [z_peers[k] for k in near] + y_peers + x_peers + [partner]
    for peer in everyone:
        pl.semaphore_signal(barrier, inc=1, device_id=peer, device_id_type=MESH)

    fetch = [
        pltpu.make_async_copy(src, dst, in_sem.at[n])
        for n, (src, dst) in enumerate(
            ((q_hbm, q_ref), (p_hbm, p_ref), (id_hbm, id_ref), (v_hbm, v_vm))
        )
    ]
    for copy in fetch:
        copy.start()
    for ref in (crecv,):
        ref[...] = jnp.full(ref.shape, NEG, F32)
    for s in range(4):
        xrecv[s * 128 + SENT : s * 128 + 128, :] = jnp.full((128 - SENT, 128), NEG, F32)
    fetch[0].wait()
    fetch[1].wait()

    zbuf[z, 12:16, :] = jnp.zeros((4, 128), jnp.bfloat16)
    for i in range(6):
        zbuf[z, 2 * i : 2 * i + 2, :] = q_ref[:, 128 * i : 128 * i + 128]
    lists = p_ref[...]
    zbuf[z, 12:14, 0:16] = lax.shift_right_logical(lists, 5).astype(F32).astype(jnp.bfloat16)
    zbuf[z, 12:14, 16:32] = (lists & 31).astype(F32).astype(jnp.bfloat16)
    pl.semaphore_wait(barrier, len(everyone))

    def remote(src, dst, send, recv, peer):
        copy = pltpu.make_async_remote_copy(
            src_ref=src, dst_ref=dst, send_sem=send, recv_sem=recv,
            device_id=peer, device_id_type=MESH,
        )
        copy.start()
        return copy

    sent = []
    z_copies = {}

    def z_send(block, k, n):
        ref = zbuf.at[(z + 16 + block) % 16]
        z_copies[n] = remote(ref, ref, zs.at[n], zr.at[n], z_peers[k])

    for k in near:
        z_send(0, k, k if k < 8 else k - 1)
    r = lax.broadcasted_iota(jnp.int32, (224, 256), 0)
    k_ = lax.broadcasted_iota(jnp.int32, (224, 256), 1)
    pick = k_ == ((r % 32) // 2) * 16 + (r // 32) * 2 + r % 2
    pick = jnp.where(pick, 1.0, 0.0).astype(jnp.bfloat16)
    for j in (1, 2, 3, 4):
        z_copies[j].wait_recv()
        z_send(-j, 4, 15 + j)
        z_copies[15 - j].wait_recv()
        if j < 4:
            z_send(j, 12, 19 + j)
    sent += list(z_copies.values())
    for n in range(16, 23):
        z_copies[n].wait_recv()
    rows = jnp.dot(pick, zbuf[...].reshape(256, 128), preferred_element_type=F32)
    rows = rows.astype(jnp.bfloat16)
    for h in range(2):
        for i in range(7):
            gath[c, x, y, h, :, 128 * i : 128 * i + 128] = rows[
                32 * i + 16 * h : 32 * i + 16 * h + 16, :
            ]

    def piece(h, back1, back2):
        if h == 0:
            return gath.at[c, (x + 4 - back2) % 4, (y + 4 - back1) % 4, h]
        return gath.at[c, (x + 4 - back1) % 4, (y + 4 - back2) % 4, h]

    peers1 = [y_peers, x_peers]
    peers2 = [x_peers, y_peers]
    first, second, cross = {}, {}, {}
    for k in range(3):
        for h in range(2):
            ref = piece(h, 0, 0)
            first[h, k] = remote(ref, ref, fs.at[h, k], fr.at[h, k], peers1[h][k])

    def forward2(h, b):
        ref = piece(h, b, 0)
        for k in range(3):
            second[h, b, k] = remote(ref, ref, ss.at[h, b, k], sr.at[h, b, k], peers2[h][k])

    def forward_core(h, b1, b2):
        ref, n = piece(h, b1, b2), b1 * 4 + b2
        cross[h, b1, b2] = remote(ref, ref, cs.at[h, n], cr.at[h, n], partner)

    for h in range(2):
        forward2(h, 0)
    for h in range(2):
        forward_core(h, 0, 0)
    for b in (1, 3, 2):
        for h in range(2):
            first[h, b - 1].wait_recv()
            forward2(h, b)
            forward_core(h, b, 0)
    for b1 in (0, 1, 3, 2):
        for b2 in (1, 3, 2):
            for h in range(2):
                second[h, b1, b2 - 1].wait_recv()
                forward_core(h, b1, b2)
    sent += list(first.values()) + list(second.values()) + list(cross.values())
    fetch[2].wait()
    fetch[3].wait()

    def score(core):
        @pl.loop(0, 2)
        def _(half):
            block = gath[core, pl.ds(half * 2, 2)].reshape(256, 896)
            turned = block[:, 768:896].astype(F32).T[:32, :].astype(jnp.int32)
            scores = lax.dot_general(
                v_vm[...], block[:, :768], (((1,), (1,)), ((), ())), preferred_element_type=F32
            )
            for t in range(2):
                s = core * 4 + half * 2 + t
                codes[pl.ds(pl.multiple_of(32 * s, 32), 32), :] = turned[:, 128 * t : 128 * t + 128]
                for j in range(64):
                    row = pl.multiple_of(j * 64 + s * 8, 8)
                    prod[pl.ds(row, 8), :] = scores[8 * j : 8 * j + 8, 128 * t : 128 * t + 128]

    score(c)
    for copy in cross.values():
        copy.wait_recv()
    score(1 - c)

    high = [codes[pl.ds(p, 8, stride=32), :] for p in range(16)]
    bits = [jnp.left_shift(jnp.int32(1), codes[pl.ds(16 + p, 8, stride=32), :]) for p in range(16)]

    @pl.loop(0, 32)
    def _(a):
        word = jnp.zeros((8, 128), jnp.int32)
        for p in range(16):
            word = word | jnp.where(high[p] == a, bits[p], 0)
        words[a] = word

    @pl.loop(0, 16)
    def _(g):
        xs = []
        for i in range(32):
            value = prod[pl.ds(g * 256 + (i // 8) * 64 + i % 8, 8, stride=8), :]
            which = id_ref[g * 32 + i]
            word = words[lax.shift_right_logical(which, 5)]
            keep = (word & jnp.left_shift(jnp.int32(1), which & 31)) != 0
            xs.append(jnp.where(keep, value, NEG))
        xs = sort_desc(xs)
        for i in range(32):
            runs[g * 32 + i] = xs[i]

    @pl.loop(0, 8)
    def _(g):
        base = g * 64
        for side, op in ((0, jnp.maximum), (1, jnp.minimum)):
            xs = [op(runs[base + i], runs[base + 63 - i]) for i in range(32)]
            xs = clean_desc(xs)
            for i in range(32):
                runs2[base + 32 * side + i] = xs[i]

    @pl.loop(0, 4)
    def _(g):
        base = g * 128
        for i in range(32):
            a, b = runs2[base + i], runs2[base + 127 - i]
            a2, b2 = runs2[base + 32 + i], runs2[base + 95 - i]
            h1, l1 = exchange(a, b)
            h2, l2 = exchange(a2, b2)
            h1, h2 = exchange(h1, h2)
            l1, l2 = exchange(l1, l2)
            runs[base + i], runs[base + 32 + i] = h1, h2
            runs[base + 64 + i], runs[base + 96 + i] = l1, l2

    @pl.loop(0, 16)
    def _(g):
        xs = clean_desc([runs[g * 32 + i] for i in range(32)])
        for i in range(32):
            runs2[g * 32 + i] = xs[i]

    def run_store(ref, base):
        def put(i, value):
            ref[base + i] = value
        return put

    def run_load(ref, base):
        return lambda i: ref[base + i]

    for g in range(2):
        merge_top(
            run_load(runs2, 256 * g), run_load(runs2, 256 * g + 128),
            run_load(runs, 256 * g), run_store(runs, 256 * g), run_store(runs2, 256 * g),
        )

    def split_store(i, value):
        csend[0, i] = value[0:4, :]
        csend[1, i] = value[4:8, :]

    merge_top(run_load(runs2, 0), run_load(runs2, 256), run_load(runs, 0), run_store(runs, 0), split_store)

    copy = remote(
        csend.at[1 - c, pl.ds(0, SENT)], crecv.at[pl.ds(0, SENT)], rcs.at[0], rcr.at[0], partner
    )
    sent.append(copy)
    copy.wait_recv()

    def x_store(i, value):
        xsend[pl.ds(i, 4, stride=128), :] = value

    merge_top(lambda i: csend[c, i], run_load(crecv, 0), run_load(ctmp, 0), run_store(ctmp, 0), x_store)

    def x_rows(s):
        return pl.ds(pl.multiple_of(s * 128, 128), SENT)

    copies = [
        remote(
            xsend.at[x_rows((x + k + 1) % 4)], xrecv.at[x_rows(x)],
            rxs.at[k], rxr.at[k], x_peers[k],
        )
        for k in range(3)
    ]
    sent += copies
    xrecv[x_rows(x), :] = xsend[x_rows(x), :]
    for copy in copies:
        copy.wait_recv()

    def pair_store(i, value):
        apair[pl.ds(i, 2, stride=128), :] = value

    merge_top(
        lambda i: xrecv[pl.ds(i, 2, stride=128), :], lambda i: xrecv[pl.ds(256 + i, 2, stride=128), :],
        run_load(atmp, 0), run_store(atmp, 0), pair_store,
    )

    def row_load(ref, base=0):
        return lambda i: ref[pl.ds(base + i, 1), :]

    def row_store(ref):
        def put(i, value):
            ref[pl.ds(i, 1), :] = value
        return put

    merge_top(row_load(apair), row_load(apair, 128), row_load(row_c), row_store(row_c), row_store(row_a))

    def fold_lanes(distance):
        row_b[...] = pltpu.roll(row_a[...], 128 - distance, axis=1)
        merge_top(row_load(row_a), row_load(row_b), row_load(row_c), row_store(row_c), row_store(row_a))

    ysend[...] = row_a[...].T

    def y_rows(s):
        return pl.ds(pl.multiple_of(s * 32, 32), 32)

    copies = [
        remote(
            ysend.at[y_rows((y + k + 1) % 4)], yrecv.at[y_rows(y)],
            rys.at[k], ryr.at[k], y_peers[k],
        )
        for k in range(3)
    ]
    sent += copies
    yrecv[y_rows(y), :] = ysend[y_rows(y), :]
    for copy in copies:
        copy.wait_recv()
    row_a[...] = yrecv[...].T
    fold_lanes(64)
    fold_lanes(32)

    turned = row_a[...].T
    for s in range(16):
        zsend[s] = turned[2 * s : 2 * s + 2, :]
    copies = [
        remote(zsend.at[(z + k + 1) % 16], zrecv.at[z], rzs.at[k], rzr.at[k], z_peers[k + 1])
        for k in range(15)
    ]
    sent += copies
    zrecv[z] = zsend[z]
    for copy in copies:
        copy.wait_recv()
    row_b[32:128, :] = jnp.full((96, 128), NEG, F32)
    for s in range(16):
        row_b[2 * s : 2 * s + 2, :] = zrecv[s]
    row_a[...] = row_b[...].T
    for distance in (16, 8, 4, 2):
        fold_lanes(distance)
    o_ref[...] = row_a[...].T[0:2, 0:K]

    for copy in sent:
        copy.wait_send()


def local(queries, probes, vectors, list_ids):
    vmem = pl.BlockSpec(memory_space=pltpu.VMEM)
    dma = pltpu.SemaphoreType.DMA
    return pl.pallas_call(
        kernel,
        out_shape=jax.ShapeDtypeStruct((2, K), F32),
        in_specs=[pl.BlockSpec(memory_space=pl.ANY)] * 4,
        out_specs=vmem,
        scratch_shapes=[
            pltpu.VMEM((2, 768), jnp.bfloat16),
            pltpu.VMEM((2, 16), jnp.int32),
            pltpu.SMEM((512,), jnp.int32),
            pltpu.VMEM((16, 16, 128), jnp.bfloat16),
            pltpu.VMEM((2, 4, 4, 2, 16, 896), jnp.bfloat16),
            pltpu.VMEM((512, 768), jnp.bfloat16),
            pltpu.VMEM((4096, 128), F32),
            pltpu.VMEM((32, 8, 128), jnp.int32),
            pltpu.VMEM((256, 128), jnp.int32),
            pltpu.VMEM((512, 8, 128), F32),
            pltpu.VMEM((512, 8, 128), F32),
            pltpu.VMEM((2, 128, 4, 128), F32),
            pltpu.VMEM((128, 4, 128), F32),
            pltpu.VMEM((128, 4, 128), F32),
            pltpu.VMEM((512, 128), F32),
            pltpu.VMEM((512, 128), F32),
            pltpu.VMEM((128, 2, 128), F32),
            pltpu.VMEM((256, 128), F32),
            pltpu.VMEM((128, 128), F32),
            pltpu.VMEM((128, 128), F32),
            pltpu.VMEM((128, 128), F32),
            pltpu.VMEM((128, 128), F32),
            pltpu.VMEM((128, 128), F32),
            pltpu.VMEM((16, 2, 128), F32),
            pltpu.VMEM((16, 2, 128), F32),
            dma((4,)), dma((23,)), dma((23,)), dma((2, 3)), dma((2, 3)), dma((2, 4, 3)), dma((2, 4, 3)),
            dma((2, 16)), dma((2, 16)), dma((1,)), dma((1,)), dma((3,)), dma((3,)),
            dma((3,)), dma((3,)), dma((15,)), dma((15,)),
        ],
        compiler_params=pltpu.CompilerParams(collective_id=0, has_side_effects=True, vmem_limit_bytes=32 * 2**20),
    )(queries, probes, vectors, list_ids)


def solution(mesh):
    return jax.shard_map(
        local,
        mesh=mesh,
        in_specs=(
            P(("pb", "dev"), None),
            P(("pb", "dev"), None),
            P(("pb", "dev"), None),
            P(("pb", "dev")),
        ),
        out_specs=P(("pb", "dev"), None),
        check_vma=False,
    )
```

```python
import functools

import jax
import jax.numpy as jnp
from jax import lax
from jax.experimental import pallas as pl
from jax.experimental.pallas import tpu as pltpu
from jax.sharding import PartitionSpec as P

K = 100
SENT = 104
NEG = -1.0e30
MESH = pl.DeviceIdType.MESH
F32 = jnp.float32


SLOT = {k % 16: n for n, k in enumerate((0, 1, 2, 3, 4, -1, -2, -3, 5, 6, 7, 8, -4, -5, -6, -7))}


def exchange(a, b):
    return jnp.maximum(a, b), jnp.minimum(a, b)


def sort_desc(xs):
    xs, n, p = list(xs), len(xs), 1
    while p < n:
        k = p
        while k >= 1:
            for j in range(k % p, n - k, 2 * k):
                for i in range(min(k, n - j - k)):
                    if (i + j) // (2 * p) == (i + j + k) // (2 * p):
                        xs[i + j], xs[i + j + k] = exchange(xs[i + j], xs[i + j + k])
            k //= 2
        p *= 2
    return xs


def clean_desc(xs):
    xs, d = list(xs), len(xs) // 2
    while d >= 1:
        for i in range(len(xs)):
            if i & d == 0:
                xs[i], xs[i + d] = exchange(xs[i], xs[i + d])
        d //= 2
    return xs


def merge_top(load_a, load_b, tmp_load, tmp_store, store):
    @pl.loop(0, 8)
    def _(g):
        for u in range(4):
            i = g * 4 + u
            m = [jnp.maximum(load_a(i + 32 * k), load_b(127 - i - 32 * k)) for k in range(4)]
            m[0], m[2] = exchange(m[0], m[2])
            m[1], m[3] = exchange(m[1], m[3])
            m[0], m[1] = exchange(m[0], m[1])
            m[2], m[3] = exchange(m[2], m[3])
            for k in range(4):
                tmp_store(i + 32 * k, m[k])

    @pl.loop(0, 4)
    def _(k):
        xs = clean_desc([tmp_load(32 * k + i) for i in range(32)])
        for i in range(32):
            store(32 * k + i, xs[i])


def kernel(
    q_hbm, p_hbm, v_hbm, id_hbm, o_ref,
    q_ref, p_ref, id_ref, zbuf, ga, gb, gc, v_vm, prod, words, codes, runs, runs2, csend, crecv, ctmp,
    xsend, xrecv, atmp, apair, row_a, row_b, row_c, dsend, drecv,
    in_sem, done, zs, zr, fs, fr, ss, sr, cs, cr, rcs, rcr, rxs, rxr, rds, rdr,
):
    pb, dev = lax.axis_index("pb"), lax.axis_index("dev")
    x, ylo, c = pb // 4, (pb // 2) % 2, pb % 2
    z, yhi = dev // 2, dev % 2
    y = yhi * 2 + ylo

    def at(x_, y_, z_, c_):
        return {"pb": x_ * 4 + (y_ % 2) * 2 + c_, "dev": z_ * 2 + y_ // 2}

    z_peers = {k: at(x, y, (z + k) % 16, c) for k in range(1, 16)}
    y_peers = [at(x, (y + k) % 4, z, c) for k in range(1, 4)]
    x_peers = [at((x + k) % 4, y, z, c) for k in range(1, 4)]
    partner = at(x, y, z, 1 - c)

    barrier = pltpu.get_barrier_semaphore()
    near = (4, 12, 3, 13, 2, 14, 1, 15)
    everyone = [z_peers[k] for k in near] + y_peers + x_peers + [partner]
    for peer in everyone:
        pl.semaphore_signal(barrier, inc=1, device_id=peer, device_id_type=MESH)

    fetch = [
        pltpu.make_async_copy(src, dst, in_sem.at[n])
        for n, (src, dst) in enumerate(
            ((q_hbm, q_ref), (p_hbm, p_ref), (id_hbm, id_ref), (v_hbm, v_vm))
        )
    ]
    for copy in fetch:
        copy.start()
    for ref in (crecv,):
        ref[...] = jnp.full(ref.shape, NEG, F32)
    for s in range(4):
        xrecv[s * 128 + SENT : s * 128 + 128, :] = jnp.full((128 - SENT, 128), NEG, F32)
    fetch[0].wait()
    fetch[1].wait()

    zbuf[0, 12:16, :] = jnp.zeros((4, 128), jnp.bfloat16)
    for i in range(6):
        zbuf[0, 2 * i : 2 * i + 2, :] = q_ref[:, 128 * i : 128 * i + 128]
    lists = p_ref[...]
    zbuf[0, 12:14, 0:16] = lax.shift_right_logical(lists, 5).astype(F32).astype(jnp.bfloat16)
    zbuf[0, 12:14, 16:32] = (lists & 31).astype(F32).astype(jnp.bfloat16)
    pl.semaphore_wait(barrier, len(everyone))

    def remote(src, dst, send, recv, peer):
        copy = pltpu.make_async_remote_copy(
            src_ref=src, dst_ref=dst, send_sem=send, recv_sem=recv,
            device_id=peer, device_id_type=MESH,
        )
        copy.start()
        return copy

    def take(ref, recv):
        pltpu.make_async_remote_copy(
            src_ref=ref, dst_ref=ref, send_sem=done.at[0], recv_sem=recv,
            device_id=partner, device_id_type=MESH,
        ).wait_recv()

    def drain(ref, send):
        pltpu.make_async_remote_copy(
            src_ref=ref, dst_ref=ref, send_sem=send, recv_sem=done.at[0],
            device_id=partner, device_id_type=MESH,
        ).wait_send()

    def z_send(block, k, n):
        remote(zbuf.at[SLOT[block % 16]], zbuf.at[SLOT[(block - k) % 16]], zs.at[0], zr.at[n], z_peers[k])

    for k in near:
        z_send(0, k, min(k, 16 - k))
    r = lax.broadcasted_iota(jnp.int32, (112, 128), 0)
    k_ = lax.broadcasted_iota(jnp.int32, (112, 128), 1)
    pick = k_ == lax.shift_right_logical(r & 15, 1) * 16 + lax.shift_right_logical(r, 4) * 2 + (r & 1)
    pick = jnp.where(pick, 1.0, 0.0).astype(jnp.bfloat16)

    def place(h):
        rows = jnp.dot(
            pick, zbuf[8 * h : 8 * h + 8].reshape(128, 128), preferred_element_type=F32
        )
        for i in range(3):
            ga[c, h, x, y, :, 128 * i : 128 * i + 128] = rows[16 * i : 16 * i + 16, :].astype(jnp.bfloat16)
            gb[c, h, y, x, :, 128 * i : 128 * i + 128] = rows[16 * i + 48 : 16 * i + 64, :].astype(jnp.bfloat16)
        return rows[96:112, :]

    kinds = [
        (lambda a2, h=h, g=g: g.at[c, h, a2], *axes)
        for h in range(2)
        for g, axes in ((ga, (x, y, y_peers, x_peers)), (gb, (y, x, x_peers, y_peers)))
    ]
    whole = [ga.at[:, 0], gb.at[:, 0], ga.at[:, 1], gb.at[:, 1], gc]
    kinds.append((lambda a2: gc.at[c, a2], x, y, y_peers, x_peers))

    def send_first(n):
        group, a2, a1, peers, _ = kinds[n]
        ref = group(a2).at[a1]
        for k in (1, 0, 2):
            remote(ref, ref, fs.at[n], fr.at[n, k], peers[k])

    def send_second(n, b):
        group, a2, a1, _, peers = kinds[n]
        ref = group(a2).at[(a1 + 4 - b) % 4]
        for k in (1, 0, 2):
            remote(ref, ref, ss.at[n], sr.at[n, k], peers[k])

    def send_cross(n, b):
        ref = kinds[n][0]((kinds[n][1] + 4 - b) % 4)
        remote(ref, ref, cs.at[n], cr.at[n], partner)

    def pass_first(which):
        for b in (1, 3, 2):
            for n in which:
                take(kinds[n][0](kinds[n][1]).at[0], fr.at[n, b - 1])
                send_second(n, b)
        for n in which:
            send_cross(n, 0)

    def pass_second(which):
        for b in (1, 3, 2):
            for n in which:
                take(kinds[n][0](kinds[n][1]), sr.at[n, b - 1])
                send_cross(n, b)

    def start(which):
        for n in which:
            send_first(n)
        for n in which:
            send_second(n, 0)

    for j in (1, 2, 3, 4):
        take(zbuf.at[0:2], zr.at[j])
        z_send(-j, 4, 0)
        if j < 4:
            z_send(j, 12, 0)
    near_codes = place(0)
    start((0, 1))
    take(zbuf.at[0:7], zr.at[0])
    far_codes = place(1)
    gc[c, x, y] = (near_codes + pltpu.roll(far_codes, 32, axis=1)).astype(jnp.bfloat16)
    start((2, 3, 4))
    pass_first((0, 1))
    pass_first((2, 3, 4))
    pass_second((0, 1))
    pass_second((2, 3, 4))

    fetch[2].wait()
    fetch[3].wait()

    def score(core):
        @pl.loop(0, 2)
        def _(half):
            block = jnp.concatenate(
                [
                    jnp.concatenate(
                        [ga[core, h, half * 2 + t].reshape(64, 384), gb[core, h, :, half * 2 + t].reshape(64, 384)],
                        axis=1,
                    )
                    for t in range(2)
                    for h in range(2)
                ],
                axis=0,
            )
            scores = lax.dot_general(
                v_vm[...], block, (((1,), (1,)), ((), ())), preferred_element_type=F32
            )
            for t in range(2):
                s = core * 4 + half * 2 + t
                turned = gc[core, half * 2 + t].reshape(64, 128).astype(F32).T.astype(jnp.int32)
                codes[pl.ds(pl.multiple_of(32 * s, 32), 32), :] = jnp.concatenate(
                    [turned[0:32, :], turned[32:64, :]], axis=1
                )
                for j in range(64):
                    row = pl.multiple_of(j * 64 + s * 8, 8)
                    prod[pl.ds(row, 8), :] = scores[8 * j : 8 * j + 8, 128 * t : 128 * t + 128]

    score(c)
    for n in range(5):
        take(whole[n].at[1 - c], cr.at[n])
    score(1 - c)

    high = [codes[pl.ds(p, 8, stride=32), :] for p in range(16)]
    bits = [jnp.left_shift(jnp.int32(1), codes[pl.ds(16 + p, 8, stride=32), :]) for p in range(16)]

    @pl.loop(0, 32)
    def _(a):
        word = jnp.zeros((8, 128), jnp.int32)
        for p in range(16):
            word = word | jnp.where(high[p] == a, bits[p], 0)
        words[a] = word

    @pl.loop(0, 16)
    def _(g):
        xs = []
        for i in range(32):
            value = prod[pl.ds(g * 256 + (i // 8) * 64 + i % 8, 8, stride=8), :]
            which = id_ref[g * 32 + i]
            word = words[lax.shift_right_logical(which, 5)]
            keep = (word & jnp.left_shift(jnp.int32(1), which & 31)) != 0
            xs.append(jnp.where(keep, value, NEG))
        xs = sort_desc(xs)
        for i in range(32):
            runs[g * 32 + i] = xs[i]

    @pl.loop(0, 8)
    def _(g):
        base = g * 64
        for side, op in ((0, jnp.maximum), (1, jnp.minimum)):
            xs = [op(runs[base + i], runs[base + 63 - i]) for i in range(32)]
            xs = clean_desc(xs)
            for i in range(32):
                runs2[base + 32 * side + i] = xs[i]

    @pl.loop(0, 4)
    def _(g):
        base = g * 128
        for i in range(32):
            a, b = runs2[base + i], runs2[base + 127 - i]
            a2, b2 = runs2[base + 32 + i], runs2[base + 95 - i]
            h1, l1 = exchange(a, b)
            h2, l2 = exchange(a2, b2)
            h1, h2 = exchange(h1, h2)
            l1, l2 = exchange(l1, l2)
            runs[base + i], runs[base + 32 + i] = h1, h2
            runs[base + 64 + i], runs[base + 96 + i] = l1, l2

    @pl.loop(0, 16)
    def _(g):
        xs = clean_desc([runs[g * 32 + i] for i in range(32)])
        for i in range(32):
            runs2[g * 32 + i] = xs[i]

    def run_store(ref, base):
        def put(i, value):
            ref[base + i] = value
        return put

    def run_load(ref, base):
        return lambda i: ref[base + i]

    for g in range(2):
        merge_top(
            run_load(runs2, 256 * g), run_load(runs2, 256 * g + 128),
            run_load(runs, 256 * g), run_store(runs, 256 * g), run_store(runs2, 256 * g),
        )

    def split_store(i, value):
        csend[0, i] = value[0:4, :]
        csend[1, i] = value[4:8, :]

    merge_top(run_load(runs2, 0), run_load(runs2, 256), run_load(runs, 0), run_store(runs, 0), split_store)

    remote(csend.at[1 - c, pl.ds(0, SENT)], crecv.at[pl.ds(0, SENT)], rcs.at[0], rcr.at[0], partner)
    take(crecv.at[pl.ds(0, SENT)], rcr.at[0])

    def x_store(i, value):
        xsend[pl.ds(i, 4, stride=128), :] = value

    merge_top(lambda i: csend[c, i], run_load(crecv, 0), run_load(ctmp, 0), run_store(ctmp, 0), x_store)

    def x_rows(s):
        return pl.ds(pl.multiple_of(s * 128, 128), SENT)

    for k in (1, 0, 2):
        remote(
            xsend.at[x_rows((x + k + 1) % 4)], xrecv.at[x_rows(x)],
            rxs.at[0], rxr.at[0], x_peers[k],
        )
    xrecv[x_rows(x), :] = xsend[x_rows(x), :]
    take(xrecv.at[pl.ds(0, 3 * SENT)], rxr.at[0])

    def pair_store(i, value):
        apair[pl.ds(i, 2, stride=128), :] = value

    merge_top(
        lambda i: xrecv[pl.ds(i, 2, stride=128), :], lambda i: xrecv[pl.ds(256 + i, 2, stride=128), :],
        run_load(atmp, 0), run_store(atmp, 0), pair_store,
    )

    def row_load(ref, base=0):
        return lambda i: ref[pl.ds(base + i, 1), :]

    def row_store(ref):
        def put(i, value):
            ref[pl.ds(i, 1), :] = value
        return put

    merge_top(row_load(apair), row_load(apair, 128), row_load(row_c), row_store(row_c), row_store(row_a))

    def fold_lanes(distance):
        row_b[...] = pltpu.roll(row_a[...], 128 - distance, axis=1)
        merge_top(row_load(row_a), row_load(row_b), row_load(row_c), row_store(row_c), row_store(row_a))

    turned = row_a[...].T
    for h in range(2):
        for y_ in range(4):
            for r8 in range(8):
                row = h * 64 + y_ * 16 + r8 * 2
                dsend[y_ * 16 + h * 8 + r8] = turned[row : row + 2, :]
    for k in (8, 7, 9, 6, 10, 5, 11, 4, 12, 3, 13, 2, 14, 1, 15, 0):
        for j in (2, 1, 3, 0):
            if (j, k) == (0, 0):
                continue
            n = j * 16 + SLOT[k]
            remote(
                dsend.at[((y + j) % 4) * 16 + SLOT[k]], drecv.at[n], rds.at[0], rdr.at[0],
                at(x, (y + j) % 4, (z + k) % 16, c),
            )
    drecv[0] = dsend[y * 16]
    take(drecv.at[1:64], rdr.at[0])
    for n in range(64):
        row_b[2 * n : 2 * n + 2, :] = drecv[n]
    row_a[...] = row_b[...].T
    for distance in (64, 32, 16, 8, 4, 2):
        fold_lanes(distance)
    o_ref[...] = row_a[...].T[0:2, 0:K]

    drain(zbuf.at[0:15], zs.at[0])
    for n in range(5):
        group, a2 = kinds[n][0], kinds[n][1]
        drain(group(a2).at[0:3], fs.at[n])
        drain(whole[n].at[c, 0:3], ss.at[n])
        drain(whole[n].at[c], cs.at[n])
    drain(crecv.at[pl.ds(0, SENT)], rcs.at[0])
    drain(xrecv.at[pl.ds(0, 3 * SENT)], rxs.at[0])
    drain(dsend.at[0:63], rds.at[0])


def local(queries, probes, vectors, list_ids):
    vmem = pl.BlockSpec(memory_space=pltpu.VMEM)
    dma = pltpu.SemaphoreType.DMA
    return pl.pallas_call(
        kernel,
        out_shape=jax.ShapeDtypeStruct((2, K), F32),
        in_specs=[pl.BlockSpec(memory_space=pltpu.HBM)] * 4,
        out_specs=vmem,
        scratch_shapes=[
            pltpu.VMEM((2, 768), jnp.bfloat16),
            pltpu.VMEM((2, 16), jnp.int32),
            pltpu.SMEM((512,), jnp.int32),
            pltpu.VMEM((16, 16, 128), jnp.bfloat16),
            pltpu.VMEM((2, 2, 4, 4, 16, 384), jnp.bfloat16),
            pltpu.VMEM((2, 2, 4, 4, 16, 384), jnp.bfloat16),
            pltpu.VMEM((2, 4, 4, 16, 128), jnp.bfloat16),
            pltpu.VMEM((512, 768), jnp.bfloat16),
            pltpu.VMEM((4096, 128), F32),
            pltpu.VMEM((32, 8, 128), jnp.int32),
            pltpu.VMEM((256, 128), jnp.int32),
            pltpu.VMEM((512, 8, 128), F32),
            pltpu.VMEM((512, 8, 128), F32),
            pltpu.VMEM((2, 128, 4, 128), F32),
            pltpu.VMEM((128, 4, 128), F32),
            pltpu.VMEM((128, 4, 128), F32),
            pltpu.VMEM((512, 128), F32),
            pltpu.VMEM((512, 128), F32),
            pltpu.VMEM((128, 2, 128), F32),
            pltpu.VMEM((256, 128), F32),
            pltpu.VMEM((128, 128), F32),
            pltpu.VMEM((128, 128), F32),
            pltpu.VMEM((128, 128), F32),
            pltpu.VMEM((64, 2, 128), F32),
            pltpu.VMEM((64, 2, 128), F32),
            dma((4,)), dma((1,)), dma((1,)), dma((5,)), dma((5,)), dma((5, 3)), dma((5,)), dma((5, 3)),
            dma((5,)), dma((5,)), dma((1,)), dma((1,)), dma((1,)), dma((1,)), dma((1,)), dma((1,)),
        ],
        compiler_params=pltpu.CompilerParams(collective_id=0, has_side_effects=True),
    )(queries, probes, vectors, list_ids)


def solution(mesh):
    return jax.shard_map(
        local,
        mesh=mesh,
        in_specs=(
            P(("pb", "dev"), None),
            P(("pb", "dev"), None),
            P(("pb", "dev"), None),
            P(("pb", "dev")),
        ),
        out_specs=P(("pb", "dev"), None),
        check_vma=False,
    )
```

```python
import functools

import jax
import jax.numpy as jnp
from jax import lax
from jax.experimental import pallas as pl
from jax.experimental.pallas import tpu as pltpu
from jax.sharding import PartitionSpec as P

K = 100
SENT = 104
NEG = -1.0e30
MESH = pl.DeviceIdType.MESH
F32 = jnp.float32


SLOT = {k % 16: n for n, k in enumerate((0, 1, 2, 3, 4, -1, -2, -3, 5, 6, 7, 8, -4, -5, -6, -7))}


def exchange(a, b):
    return jnp.maximum(a, b), jnp.minimum(a, b)


def sort_desc(xs):
    xs, n, p = list(xs), len(xs), 1
    while p < n:
        k = p
        while k >= 1:
            for j in range(k % p, n - k, 2 * k):
                for i in range(min(k, n - j - k)):
                    if (i + j) // (2 * p) == (i + j + k) // (2 * p):
                        xs[i + j], xs[i + j + k] = exchange(xs[i + j], xs[i + j + k])
            k //= 2
        p *= 2
    return xs


def clean_desc(xs):
    xs, d = list(xs), len(xs) // 2
    while d >= 1:
        for i in range(len(xs)):
            if i & d == 0:
                xs[i], xs[i + d] = exchange(xs[i], xs[i + d])
        d //= 2
    return xs


def clean_rows(xs, up=None):
    def order(hi, lo):
        if up is None:
            return hi, lo
        if up is True:
            return lo, hi
        return jnp.where(up, lo, hi), jnp.where(up, hi, lo)

    xs = list(xs)
    for d in (8, 4, 2, 1):
        for i in range(16):
            if i & d == 0:
                xs[i], xs[i + d] = order(*exchange(xs[i], xs[i + d]))
    row = lax.broadcasted_iota(jnp.int32, (8, 128), 0)
    for d in (4, 2, 1):
        lower = (row & d) == 0
        if up is None:
            larger = lower
        elif up is True:
            larger = (row & d) != 0
        else:
            larger = lower != up
        for i in range(16):
            if d == 4:
                other = pltpu.roll(xs[i], 4, axis=0)
            else:
                other = jnp.where(lower, pltpu.roll(xs[i], 8 - d, axis=0), pltpu.roll(xs[i], d, axis=0))
            hi, lo = exchange(xs[i], other)
            xs[i] = jnp.where(larger, hi, lo)
    return xs


def merge_top(load_a, load_b, tmp_load, tmp_store, store):
    @pl.loop(0, 8)
    def _(g):
        for u in range(4):
            i = g * 4 + u
            m = [jnp.maximum(load_a(i + 32 * k), load_b(127 - i - 32 * k)) for k in range(4)]
            m[0], m[2] = exchange(m[0], m[2])
            m[1], m[3] = exchange(m[1], m[3])
            m[0], m[1] = exchange(m[0], m[1])
            m[2], m[3] = exchange(m[2], m[3])
            for k in range(4):
                tmp_store(i + 32 * k, m[k])

    @pl.loop(0, 4)
    def _(k):
        xs = clean_desc([tmp_load(32 * k + i) for i in range(32)])
        for i in range(32):
            store(32 * k + i, xs[i])


def kernel(
    q_hbm, p_hbm, v_hbm, id_hbm, o_ref,
    q_ref, p_ref, ids, row_of, bit_of, rows1, bits1, rows2, bits2, zbuf, ga, gb, gc, v_vm, prod, words, words2, codes, runs, runs2, ctmp,
    xsend, xrecv, row_a, row_b, dsend, drecv,
    in_sem, done, vs, vr, zs, zr, fs, fr, ss, sr, rxs, rxr, rds, rdr,
):
    pb, dev = lax.axis_index("pb"), lax.axis_index("dev")
    x, ylo, c = pb // 4, (pb // 2) % 2, pb % 2
    z, yhi = dev // 2, dev % 2
    y = yhi * 2 + ylo

    def at(x_, y_, z_, c_):
        return {"pb": x_ * 4 + (y_ % 2) * 2 + c_, "dev": z_ * 2 + y_ // 2}

    z_peers = {k: at(x, y, (z + k) % 16, c) for k in range(1, 16)}
    y_peers = [at(x, (y + k) % 4, z, c) for k in range(1, 4)]
    x_peers = [at((x + k) % 4, y, z, c) for k in range(1, 4)]
    partner = at(x, y, z, 1 - c)

    barrier = pltpu.get_barrier_semaphore()
    near = (4, 12, 3, 13, 2, 14, 1, 15)
    everyone = [z_peers[k] for k in near] + y_peers + x_peers + [partner]
    for peer in everyone:
        pl.semaphore_signal(barrier, inc=1, device_id=peer, device_id_type=MESH)

    fetch = [
        pltpu.make_async_copy(src, dst, in_sem.at[n])
        for n, (src, dst) in enumerate(
            ((q_hbm, q_ref), (p_hbm, p_ref), (id_hbm, ids), (v_hbm, v_vm.at[0]))
        )
    ]
    for copy in fetch:
        copy.start()
    for s in range(4):
        pad = s * 128 + (0 if s % 2 else SENT)
        xrecv[pad : pad + 128 - SENT, :] = jnp.full((128 - SENT, 128), NEG, F32)
    fetch[0].wait()
    fetch[1].wait()

    zbuf[0, 12:16, :] = jnp.zeros((4, 128), jnp.bfloat16)
    for i in range(6):
        zbuf[0, 2 * i : 2 * i + 2, :] = q_ref[:, 128 * i : 128 * i + 128]
    lists = p_ref[...]
    zbuf[0, 12:14, 0:16] = lax.shift_right_logical(lists, 5).astype(F32).astype(jnp.bfloat16)
    zbuf[0, 12:14, 16:32] = (lists & 31).astype(F32).astype(jnp.bfloat16)
    pl.semaphore_wait(barrier, len(everyone))

    def remote(src, dst, send, recv, peer):
        copy = pltpu.make_async_remote_copy(
            src_ref=src, dst_ref=dst, send_sem=send, recv_sem=recv,
            device_id=peer, device_id_type=MESH,
        )
        copy.start()
        return copy

    def take(ref, recv):
        pltpu.make_async_remote_copy(
            src_ref=ref, dst_ref=ref, send_sem=done.at[0], recv_sem=recv,
            device_id=partner, device_id_type=MESH,
        ).wait_recv()

    def drain(ref, send):
        pltpu.make_async_remote_copy(
            src_ref=ref, dst_ref=ref, send_sem=send, recv_sem=done.at[0],
            device_id=partner, device_id_type=MESH,
        ).wait_send()

    def z_send(block, k, n):
        remote(zbuf.at[SLOT[block % 16]], zbuf.at[SLOT[(block - k) % 16]], zs.at[0], zr.at[n], z_peers[k])

    for k in near:
        z_send(0, k, min(k, 16 - k))
    remote(v_hbm, v_vm.at[1], vs.at[0], vr.at[0], partner)
    fetch[2].wait()
    row_of[...] = lax.shift_right_logical(ids[...], 5)
    bit_of[...] = jnp.left_shift(jnp.int32(1), ids[...] & 31)
    tables = [
        pltpu.make_async_copy(row_of, rows1, in_sem.at[4]), pltpu.make_async_copy(bit_of, bits1, in_sem.at[5])
    ]
    for copy in tables:
        copy.start()
    remote(row_of, rows2, vs.at[1], vr.at[1], partner)
    remote(bit_of, bits2, vs.at[2], vr.at[2], partner)
    r = lax.broadcasted_iota(jnp.int32, (112, 128), 0)
    k_ = lax.broadcasted_iota(jnp.int32, (112, 128), 1)
    pick = k_ == lax.shift_right_logical(r & 15, 1) * 16 + lax.shift_right_logical(r, 4) * 2 + (r & 1)
    pick = jnp.where(pick, 1.0, 0.0).astype(jnp.bfloat16)

    def place(h):
        rows = jnp.dot(
            pick, zbuf[8 * h : 8 * h + 8].reshape(128, 128), preferred_element_type=F32
        )
        for i in range(3):
            ga[h, x, y, :, 128 * i : 128 * i + 128] = rows[16 * i : 16 * i + 16, :].astype(jnp.bfloat16)
            gb[h, y, x, :, 128 * i : 128 * i + 128] = rows[16 * i + 48 : 16 * i + 64, :].astype(jnp.bfloat16)
        return rows[96:112, :]

    kinds = [
        (lambda a2, h=h, g=g: g.at[h, a2], *axes)
        for h in range(2)
        for g, axes in ((ga, (x, y, y_peers, x_peers)), (gb, (y, x, x_peers, y_peers)))
    ]
    whole = [ga.at[0], gb.at[0], ga.at[1], gb.at[1], gc]
    kinds.append((lambda a2: gc.at[a2], x, y, y_peers, x_peers))

    def send_first(n):
        group, a2, a1, peers, _ = kinds[n]
        ref = group(a2).at[a1]
        for k in (1, 0, 2):
            remote(ref, ref, fs.at[n], fr.at[n, k], peers[k])

    def send_second(n, b):
        group, a2, a1, _, peers = kinds[n]
        ref = group(a2).at[(a1 + 4 - b) % 4]
        for k in (1, 0, 2):
            remote(ref, ref, ss.at[n], sr.at[n, k], peers[k])

    def pass_first(which):
        for b in (1, 3, 2):
            for n in which:
                take(kinds[n][0](kinds[n][1]).at[0], fr.at[n, b - 1])
                send_second(n, b)

    def pass_second(which):
        for b in (1, 3, 2):
            for n in which:
                take(kinds[n][0](kinds[n][1]), sr.at[n, b - 1])

    def start(which):
        for n in which:
            send_first(n)
        for n in which:
            send_second(n, 0)

    for j in (1, 2, 3, 4):
        take(zbuf.at[0:2], zr.at[j])
        z_send(-j, 4, 0)
        if j < 4:
            z_send(j, 12, 0)
    near_codes = place(0)
    start((0, 1))
    take(zbuf.at[0:7], zr.at[0])
    far_codes = place(1)
    gc[x, y] = (near_codes + pltpu.roll(far_codes, 32, axis=1)).astype(jnp.bfloat16)
    start((4, 2, 3))
    pass_first((0, 1))
    pass_first((4, 2, 3))
    pass_second((0, 1))
    fetch[3].wait()
    for copy in tables:
        copy.wait()
    take(v_vm.at[1], vr.at[0])
    take(rows2, vr.at[1])
    take(bits2, vr.at[2])

    def score(h):
        block = jnp.concatenate(
            [
                jnp.concatenate([ga[h, s].reshape(64, 384), gb[h, :, s].reshape(64, 384)], axis=1)
                for s in range(4)
            ],
            axis=0,
        )

        @pl.loop(0, 2)
        def _(core):
            scores = lax.dot_general(
                v_vm[core], block, (((1,), (1,)), ((), ())), preferred_element_type=F32
            )
            for s in range(4):
                part = scores[:, 128 * (s // 2) : 128 * (s // 2) + 128]
                if s % 2 != h:
                    part = pltpu.roll(part, 64, axis=1)
                for j in range(64):
                    row = pl.multiple_of(j * 64 + (core * 4 + s) * 8, 8)
                    prod[pl.ds(row, 8), 64 * h : 64 * h + 64] = part[
                        8 * j : 8 * j + 8, 64 * h : 64 * h + 64
                    ]

    score(0)
    pass_second((4, 2, 3))
    score(1)
    for s in range(4):
        turned = gc[s].reshape(64, 128).astype(F32).T.astype(jnp.int32)
        turned = jnp.concatenate([turned[0:32, :], turned[32:64, :]], axis=1)
        codes[32 * s : 32 * s + 32, :] = turned
        codes[32 * s + 128 : 32 * s + 160, :] = turned
    high = [codes[pl.ds(p, 8, stride=32), :] for p in range(16)]
    bits = [jnp.left_shift(jnp.int32(1), codes[pl.ds(16 + p, 8, stride=32), :]) for p in range(16)]
    own = lax.broadcasted_iota(jnp.int32, (8, 128), 0) < 4

    @pl.loop(0, 8)
    def _(a4):
        for a in range(4):
            terms = [jnp.where(high[p] == a4 * 4 + a, bits[p], 0) for p in range(16)]
            while len(terms) > 1:
                terms = [terms[i] | terms[i + 1] for i in range(0, len(terms), 2)]
            words[a4 * 4 + a] = jnp.where(own, terms[0], 0)
            words2[a4 * 4 + a] = jnp.where(own, 0, terms[0])

    @pl.loop(0, 16)
    def _(g):
        xs = []
        for i in range(32):
            value = prod[pl.ds(g * 256 + (i // 8) * 64 + i % 8, 8, stride=8), :]
            found = []
            for row_ref, bit_ref, table in ((rows1, bits1, words), (rows2, bits2, words2)):
                word = table[row_ref[g * 32 + i]]
                found.append(word & bit_ref[g * 32 + i])
            xs.append(jnp.where((found[0] | found[1]) != 0, value, NEG))
        xs = sort_desc(xs)
        for i in range(32):
            runs[g * 32 + i] = xs[i]

    @pl.loop(0, 8)
    def _(g):
        base = g * 64
        for side, op in ((0, jnp.maximum), (1, jnp.minimum)):
            xs = [op(runs[base + i], runs[base + 63 - i]) for i in range(32)]
            xs = clean_desc(xs)
            for i in range(32):
                runs2[base + 32 * side + i] = xs[i]

    @pl.loop(0, 4)
    def _(g):
        base = g * 128
        for i in range(32):
            a, b = runs2[base + i], runs2[base + 127 - i]
            a2, b2 = runs2[base + 32 + i], runs2[base + 95 - i]
            h1, l1 = exchange(a, b)
            h2, l2 = exchange(a2, b2)
            h1, h2 = exchange(h1, h2)
            l1, l2 = exchange(l1, l2)
            runs[base + i], runs[base + 32 + i] = h1, h2
            runs[base + 64 + i], runs[base + 96 + i] = l1, l2

    @pl.loop(0, 16)
    def _(g):
        xs = clean_desc([runs[g * 32 + i] for i in range(32)])
        for i in range(32):
            runs2[g * 32 + i] = xs[i]

    def run_store(ref, base):
        def put(i, value):
            ref[base + i] = value
        return put

    def run_load(ref, base):
        return lambda i: ref[base + i]

    for g in range(2):
        merge_top(
            run_load(runs2, 256 * g), run_load(runs2, 256 * g + 128),
            run_load(runs, 256 * g), run_store(runs, 256 * g), run_store(runs2, 256 * g),
        )

    merge_top(
        run_load(runs2, 0), run_load(runs2, 256), run_load(runs, 0), run_store(runs, 0), run_store(runs2, 0)
    )

    def x_store(i, value):
        xsend[pl.ds(i + (x & 1) * (127 - 2 * i), 4, stride=128), :] = value

    merge_top(
        lambda i: runs2[i, 0:4, :], lambda i: runs2[i, 4:8, :], run_load(ctmp, 0), run_store(ctmp, 0), x_store
    )

    def x_rows(s):
        return pl.ds(pl.multiple_of(s * 128 + (x & 1) * (128 - SENT), 8), SENT)

    for k in (1, 0, 2):
        remote(
            xsend.at[x_rows((x + k + 1) % 4)], xrecv.at[x_rows(x)],
            rxs.at[0], rxr.at[0], x_peers[k],
        )
    xrecv[x_rows(x), :] = xsend[x_rows(x), :]
    take(xrecv.at[pl.ds(0, 3 * SENT)], rxr.at[0])

    def blocks(ref, base=0):
        return [ref[base + 8 * i : base + 8 * i + 8, :] for i in range(16)]

    def join(xs, ys):
        return [jnp.maximum(a, b) for a, b in zip(xs, ys)]

    lane = lax.broadcasted_iota(jnp.int32, (8, 128), 1)
    low = clean_rows(join(blocks(xrecv), blocks(xrecv, 128)))
    high = clean_rows(join(blocks(xrecv, 256), blocks(xrecv, 384)), True)
    up = ((lax.shift_right_logical(lane, 4) + 4 - y) & 3) >= 2
    merged = clean_rows(join(low, high), up)

    turned = jnp.concatenate(merged, axis=0).T
    for h in range(2):
        for y_ in range(4):
            for r8 in range(8):
                row = h * 64 + y_ * 16 + r8 * 2
                dsend[y_ * 16 + h * 8 + r8] = turned[row : row + 2, :]
    for k in (8, 7, 9, 6, 10, 5, 11, 4, 12, 3, 13, 2, 14, 1, 15, 0):
        for j in (2, 1, 3, 0):
            if (j, k) == (0, 0):
                continue
            n = j * 16 + SLOT[k]
            remote(
                dsend.at[((y + j) % 4) * 16 + SLOT[k]], drecv.at[n], rds.at[0], rdr.at[0],
                at(x, (y + j) % 4, (z + k) % 16, c),
            )
    drecv[0] = dsend[y * 16]
    take(drecv.at[1:64], rdr.at[0])
    for n in range(64):
        row_b[2 * n : 2 * n + 2, :] = drecv[n]
    row_a[...] = row_b[...].T
    merged = blocks(row_a)
    for distance in (64, 32, 16, 8, 4, 2):
        merged = join(merged, [pltpu.roll(v, 128 - distance, axis=1) for v in merged])
        up = (lane & (distance // 2)) != 0 if distance > 2 else None
        merged = clean_rows(merged, up)
    o_ref[...] = jnp.concatenate(merged, axis=0).T[0:2, 0:K]

    drain(zbuf.at[0:15], zs.at[0])
    for n in range(5):
        group, a2 = kinds[n][0], kinds[n][1]
        drain(group(a2).at[0:3], fs.at[n])
        drain(whole[n].at[0:3], ss.at[n])
    drain(v_vm.at[1], vs.at[0])
    drain(row_of, vs.at[1])
    drain(bit_of, vs.at[2])
    drain(xrecv.at[pl.ds(0, 3 * SENT)], rxs.at[0])
    drain(dsend.at[0:63], rds.at[0])


def local(queries, probes, vectors, list_ids):
    vmem = pl.BlockSpec(memory_space=pltpu.VMEM)
    dma = pltpu.SemaphoreType.DMA
    return pl.pallas_call(
        kernel,
        out_shape=jax.ShapeDtypeStruct((2, K), F32),
        in_specs=[pl.BlockSpec(memory_space=pltpu.HBM)] * 4,
        out_specs=vmem,
        scratch_shapes=[
            pltpu.VMEM((2, 768), jnp.bfloat16),
            pltpu.VMEM((2, 16), jnp.int32),
            pltpu.VMEM((512,), jnp.int32),
            pltpu.VMEM((512,), jnp.int32),
            pltpu.VMEM((512,), jnp.int32),
            pltpu.SMEM((512,), jnp.int32),
            pltpu.SMEM((512,), jnp.int32),
            pltpu.SMEM((512,), jnp.int32),
            pltpu.SMEM((512,), jnp.int32),
            pltpu.VMEM((16, 16, 128), jnp.bfloat16),
            pltpu.VMEM((2, 4, 4, 16, 384), jnp.bfloat16),
            pltpu.VMEM((2, 4, 4, 16, 384), jnp.bfloat16),
            pltpu.VMEM((4, 4, 16, 128), jnp.bfloat16),
            pltpu.VMEM((2, 512, 768), jnp.bfloat16),
            pltpu.VMEM((4096, 128), F32),
            pltpu.VMEM((32, 8, 128), jnp.int32),
            pltpu.VMEM((32, 8, 128), jnp.int32),
            pltpu.VMEM((256, 128), jnp.int32),
            pltpu.VMEM((512, 8, 128), F32),
            pltpu.VMEM((512, 8, 128), F32),
            pltpu.VMEM((128, 4, 128), F32),
            pltpu.VMEM((512, 128), F32),
            pltpu.VMEM((512, 128), F32),
            pltpu.VMEM((128, 128), F32),
            pltpu.VMEM((128, 128), F32),
            pltpu.VMEM((64, 2, 128), F32),
            pltpu.VMEM((64, 2, 128), F32),
            dma((6,)), dma((1,)), dma((3,)), dma((3,)), dma((1,)), dma((5,)), dma((5,)), dma((5, 3)), dma((5,)),
            dma((5, 3)), dma((1,)), dma((1,)), dma((1,)), dma((1,)),
        ],
        compiler_params=pltpu.CompilerParams(collective_id=0, has_side_effects=True),
    )(queries, probes, vectors, list_ids)


def solution(mesh):
    return jax.shard_map(
        local,
        mesh=mesh,
        in_specs=(
            P(("pb", "dev"), None),
            P(("pb", "dev"), None),
            P(("pb", "dev"), None),
            P(("pb", "dev")),
        ),
        out_specs=P(("pb", "dev"), None),
        check_vma=False,
    )
```

```python
import functools

import jax
import jax.numpy as jnp
from jax import lax
from jax.experimental import pallas as pl
from jax.experimental.pallas import tpu as pltpu
from jax.sharding import PartitionSpec as P

K = 100
SENT = 104
NEG = -1.0e30
MESH = pl.DeviceIdType.MESH
F32 = jnp.float32


SLOT = {k % 16: n for n, k in enumerate((0, 1, 2, 3, 4, -1, -2, -3, 5, 6, 7, 8, -4, -5, -6, -7))}


def exchange(a, b):
    return jnp.maximum(a, b), jnp.minimum(a, b)


def sort_desc(xs):
    xs, n, p = list(xs), len(xs), 1
    while p < n:
        k = p
        while k >= 1:
            for j in range(k % p, n - k, 2 * k):
                for i in range(min(k, n - j - k)):
                    if (i + j) // (2 * p) == (i + j + k) // (2 * p):
                        xs[i + j], xs[i + j + k] = exchange(xs[i + j], xs[i + j + k])
            k //= 2
        p *= 2
    return xs


def clean_desc(xs):
    xs, d = list(xs), len(xs) // 2
    while d >= 1:
        for i in range(len(xs)):
            if i & d == 0:
                xs[i], xs[i + d] = exchange(xs[i], xs[i + d])
        d //= 2
    return xs


def clean_rows(xs, up=None):
    def order(hi, lo):
        if up is None:
            return hi, lo
        if up is True:
            return lo, hi
        return jnp.where(up, lo, hi), jnp.where(up, hi, lo)

    xs = list(xs)
    for d in (8, 4, 2, 1):
        for i in range(16):
            if i & d == 0:
                xs[i], xs[i + d] = order(*exchange(xs[i], xs[i + d]))
    row = lax.broadcasted_iota(jnp.int32, (8, 128), 0)
    for d in (4, 2, 1):
        lower = (row & d) == 0
        if up is None:
            larger = lower
        elif up is True:
            larger = (row & d) != 0
        else:
            larger = lower != up
        for i in range(16):
            if d == 4:
                other = pltpu.roll(xs[i], 4, axis=0)
            else:
                other = jnp.where(lower, pltpu.roll(xs[i], 8 - d, axis=0), pltpu.roll(xs[i], d, axis=0))
            hi, lo = exchange(xs[i], other)
            xs[i] = jnp.where(larger, hi, lo)
    return xs


def merge_top(load_a, load_b, tmp_load, tmp_store, store, after=None):
    @pl.loop(0, 2)
    def _(g):
        for u in range(16):
            i = g * 16 + u
            m = [jnp.maximum(load_a(i + 32 * k), load_b(127 - i - 32 * k)) for k in range(4)]
            m[0], m[2] = exchange(m[0], m[2])
            m[1], m[3] = exchange(m[1], m[3])
            m[0], m[1] = exchange(m[0], m[1])
            m[2], m[3] = exchange(m[2], m[3])
            for k in range(4):
                tmp_store(i + 32 * k, m[k])

    def finish(k):
        xs = clean_desc([tmp_load(32 * k + i) for i in range(32)])
        for i in range(32):
            store(32 * k + i, xs[i])

    if after is None:
        pl.loop(0, 4)(finish)
    else:
        for k in range(4):
            finish(k)
            after(k)


def kernel(
    q_hbm, p_hbm, v_hbm, id_hbm, flat_hbm, o_ref,
    q_ref, p_ref, ids, ids2, flat, row_of, rows1, rows2, bit_of, zbuf, ga, gb, gc, v_vm, prod, words, words2, codes, runs, runs2, ctmp,
    xsend, xrecv, row_a, row_b, dsend, drecv,
    in_sem, done, vs, vr, zs, zr, fs, fr, ss, sr, rxs, rxr, rds, rdr,
):
    pb, dev = lax.axis_index("pb"), lax.axis_index("dev")
    x, ylo, c = pb // 4, (pb // 2) % 2, pb % 2
    z, yhi = dev // 2, dev % 2
    y = yhi * 2 + ylo

    def at(x_, y_, z_, c_):
        return {"pb": x_ * 4 + (y_ % 2) * 2 + c_, "dev": z_ * 2 + y_ // 2}

    z_peers = {k: at(x, y, (z + k) % 16, c) for k in range(1, 16)}
    y_peers = [at(x, (y + k) % 4, z, c) for k in range(1, 4)]
    x_peers = [at((x + k) % 4, y, z, c) for k in range(1, 4)]
    partner = at(x, y, z, 1 - c)

    barrier = pltpu.get_barrier_semaphore()
    near = (4, 12, 3, 13, 2, 14, 1, 15)
    everyone = [z_peers[k] for k in near] + y_peers + x_peers + [partner]
    for peer in everyone:
        pl.semaphore_signal(barrier, inc=1, device_id=peer, device_id_type=MESH)

    fetch = [
        pltpu.make_async_copy(src, dst, in_sem.at[n])
        for n, (src, dst) in enumerate(
            ((q_hbm, q_ref), (p_hbm, p_ref), (id_hbm, ids), (v_hbm, v_vm.at[0]), (flat_hbm, flat))
        )
    ]
    for copy in fetch:
        copy.start()
    for s in range(4):
        pad = s * 128 + (0 if s % 2 else SENT)
        xrecv[pad : pad + 128 - SENT, :] = jnp.full((128 - SENT, 128), NEG, F32)
    fetch[0].wait()
    fetch[1].wait()

    zbuf[0, 12:16, :] = jnp.zeros((4, 128), jnp.bfloat16)
    for i in range(6):
        zbuf[0, 2 * i : 2 * i + 2, :] = q_ref[:, 128 * i : 128 * i + 128]
    lists = p_ref[...]
    zbuf[0, 12:14, 0:16] = lax.shift_right_logical(lists, 5).astype(F32).astype(jnp.bfloat16)
    zbuf[0, 12:14, 16:32] = (lists & 31).astype(F32).astype(jnp.bfloat16)
    pl.semaphore_wait(barrier, len(everyone))

    def remote(src, dst, send, recv, peer):
        copy = pltpu.make_async_remote_copy(
            src_ref=src, dst_ref=dst, send_sem=send, recv_sem=recv,
            device_id=peer, device_id_type=MESH,
        )
        copy.start()
        return copy

    def take(ref, recv):
        pltpu.make_async_remote_copy(
            src_ref=ref, dst_ref=ref, send_sem=done.at[0], recv_sem=recv,
            device_id=partner, device_id_type=MESH,
        ).wait_recv()

    def drain(ref, send):
        pltpu.make_async_remote_copy(
            src_ref=ref, dst_ref=ref, send_sem=send, recv_sem=done.at[0],
            device_id=partner, device_id_type=MESH,
        ).wait_send()

    def z_send(block, k, n):
        remote(zbuf.at[SLOT[block % 16]], zbuf.at[SLOT[(block - k) % 16]], zs.at[0], zr.at[n], z_peers[k])

    for k in near:
        z_send(0, k, min(k, 16 - k))
    remote(v_hbm, v_vm.at[1], vs.at[0], vr.at[0], partner)
    fetch[2].wait()
    fetch[4].wait()
    row_of[...] = lax.shift_right_logical(flat[...], 5)
    table = pltpu.make_async_copy(row_of, rows1, in_sem.at[5])
    table.start()
    remote(row_of, rows2, vs.at[1], vr.at[1], partner)
    remote(ids, ids2, vs.at[2], vr.at[2], partner)
    r = lax.broadcasted_iota(jnp.int32, (112, 128), 0)
    k_ = lax.broadcasted_iota(jnp.int32, (112, 128), 1)
    pick = k_ == lax.shift_right_logical(r & 15, 1) * 16 + lax.shift_right_logical(r, 4) * 2 + (r & 1)
    pick = jnp.where(pick, 1.0, 0.0).astype(jnp.bfloat16)

    def place(h):
        rows = jnp.dot(
            pick, zbuf[8 * h : 8 * h + 8].reshape(128, 128), preferred_element_type=F32
        )
        for i in range(3):
            ga[h, x, y, :, 128 * i : 128 * i + 128] = rows[16 * i : 16 * i + 16, :].astype(jnp.bfloat16)
            gb[h, y, x, :, 128 * i : 128 * i + 128] = rows[16 * i + 48 : 16 * i + 64, :].astype(jnp.bfloat16)
        return rows[96:112, :]

    kinds = [
        (lambda a2, h=h, g=g: g.at[h, a2], *axes)
        for h in range(2)
        for g, axes in ((ga, (x, y, y_peers, x_peers)), (gb, (y, x, x_peers, y_peers)))
    ]
    whole = [ga.at[0], gb.at[0], ga.at[1], gb.at[1], gc]
    kinds.append((lambda a2: gc.at[a2], x, y, y_peers, x_peers))

    def send_first(n):
        group, a2, a1, peers, _ = kinds[n]
        ref = group(a2).at[a1]
        for k in (1, 0, 2):
            remote(ref, ref, fs.at[n], fr.at[n, k], peers[k])

    def send_second(n, b):
        group, a2, a1, _, peers = kinds[n]
        ref = group(a2).at[(a1 + 4 - b) % 4]
        for k in (1, 0, 2):
            remote(ref, ref, ss.at[n], sr.at[n, k], peers[k])

    def pass_first(which):
        for b in (1, 3, 2):
            for n in which:
                take(kinds[n][0](kinds[n][1]).at[0], fr.at[n, b - 1])
                send_second(n, b)

    def pass_second(which):
        for b in (1, 3, 2):
            for n in which:
                take(kinds[n][0](kinds[n][1]), sr.at[n, b - 1])

    def start(which):
        for n in which:
            send_first(n)
        for n in which:
            send_second(n, 0)

    for j in (1, 2, 3, 4):
        take(zbuf.at[0:2], zr.at[j])
        z_send(-j, 4, 0)
        if j < 4:
            z_send(j, 12, 0)
    near_codes = place(0)
    start((0, 1))

    take(ids2, vr.at[2])
    for part in range(4):
        for s, ref in enumerate((ids, ids2)):
            column = jnp.broadcast_to(ref[part : part + 1, :], (128, 128)).T
            bit = jnp.left_shift(jnp.int32(1), column & 31)
            for t in range(4):
                bit_of[pl.ds(part * 1024 + 4 * s + t, 128, stride=8), :] = bit

    take(zbuf.at[0:7], zr.at[0])
    far_codes = place(1)
    gc[x, y] = (near_codes + pltpu.roll(far_codes, 32, axis=1)).astype(jnp.bfloat16)
    start((4, 2, 3))
    pass_first((0, 1))
    pass_first((4, 2, 3))
    pass_second((0, 1))
    fetch[3].wait()
    table.wait()
    take(v_vm.at[1], vr.at[0])
    take(rows2, vr.at[1])

    def score(h):
        block = jnp.concatenate(
            [
                jnp.concatenate([ga[h, s].reshape(64, 384), gb[h, :, s].reshape(64, 384)], axis=1)
                for s in range(4)
            ],
            axis=0,
        )

        @pl.loop(0, 2)
        def _(core):
            scores = lax.dot_general(
                v_vm[core], block, (((1,), (1,)), ((), ())), preferred_element_type=F32
            )
            for s in range(4):
                part = scores[:, 128 * (s // 2) : 128 * (s // 2) + 128]
                if s % 2 != h:
                    part = pltpu.roll(part, 64, axis=1)
                for j in range(64):
                    row = pl.multiple_of(j * 64 + (core * 4 + s) * 8, 8)
                    prod[pl.ds(row, 8), 64 * h : 64 * h + 64] = part[
                        8 * j : 8 * j + 8, 64 * h : 64 * h + 64
                    ]

    score(0)
    pass_second((4,))
    for s in range(4):
        turned = gc[s].reshape(64, 128).astype(F32).T.astype(jnp.int32)
        turned = jnp.concatenate([turned[0:32, :], turned[32:64, :]], axis=1)
        codes[32 * s : 32 * s + 32, :] = turned
        codes[32 * s + 128 : 32 * s + 160, :] = turned
    high = [codes[pl.ds(p, 8, stride=32), :] for p in range(16)]
    bits = [jnp.left_shift(jnp.int32(1), codes[pl.ds(16 + p, 8, stride=32), :]) for p in range(16)]
    own = lax.broadcasted_iota(jnp.int32, (8, 128), 0) < 4

    @pl.loop(0, 8)
    def _(a4):
        for a in range(4):
            terms = [jnp.where(high[p] == a4 * 4 + a, bits[p], 0) for p in range(16)]
            while len(terms) > 1:
                terms = [terms[i] | terms[i + 1] for i in range(0, len(terms), 2)]
            words[a4 * 4 + a] = jnp.where(own, terms[0], 0)
            words2[a4 * 4 + a] = jnp.where(own, 0, terms[0])

    pass_second((2, 3))
    score(1)

    @pl.loop(0, 16)
    def _(g):
        xs = []
        for i in range(32):
            value = prod[pl.ds(g * 256 + (i // 8) * 64 + i % 8, 8, stride=8), :]
            word = words[rows1[g * 32 + i]] | words2[rows2[g * 32 + i]]
            found = word & bit_of[pl.ds(pl.multiple_of(g * 256 + i * 8, 8), 8), :]
            xs.append(jnp.where(found != 0, value, NEG))
        xs = sort_desc(xs)
        for i in range(32):
            runs[g * 32 + i] = xs[i]

    @pl.loop(0, 8)
    def _(g):
        base = g * 64
        for side, op in ((0, jnp.maximum), (1, jnp.minimum)):
            xs = [op(runs[base + i], runs[base + 63 - i]) for i in range(32)]
            xs = clean_desc(xs)
            for i in range(32):
                runs2[base + 32 * side + i] = xs[i]

    @pl.loop(0, 4)
    def _(g):
        base = g * 128
        for i in range(32):
            a, b = runs2[base + i], runs2[base + 127 - i]
            a2, b2 = runs2[base + 32 + i], runs2[base + 95 - i]
            h1, l1 = exchange(a, b)
            h2, l2 = exchange(a2, b2)
            h1, h2 = exchange(h1, h2)
            l1, l2 = exchange(l1, l2)
            runs[base + i], runs[base + 32 + i] = h1, h2
            runs[base + 64 + i], runs[base + 96 + i] = l1, l2

    @pl.loop(0, 16)
    def _(g):
        xs = clean_desc([runs[g * 32 + i] for i in range(32)])
        for i in range(32):
            runs2[g * 32 + i] = xs[i]

    def run_store(ref, base):
        def put(i, value):
            ref[base + i] = value
        return put

    def run_load(ref, base):
        return lambda i: ref[base + i]

    for g in range(2):
        merge_top(
            run_load(runs2, 256 * g), run_load(runs2, 256 * g + 128),
            run_load(runs, 256 * g), run_store(runs, 256 * g), run_store(runs2, 256 * g),
        )

    merge_top(
        run_load(runs2, 0), run_load(runs2, 256), run_load(runs, 0), run_store(runs, 0), run_store(runs2, 0)
    )

    def x_store(i, value):
        xsend[pl.ds(i + (x & 1) * (127 - 2 * i), 4, stride=128), :] = value

    def x_rows(s, start, size):
        ascending = 128 - size - start
        return pl.ds(pl.multiple_of(s * 128 + start + (x & 1) * (ascending - start), 8), size)

    def x_send(q):
        start, size = 32 * q, min(32, SENT - 32 * q)
        for k in (1, 0, 2):
            remote(
                xsend.at[x_rows((x + k + 1) % 4, start, size)], xrecv.at[x_rows(x, start, size)],
                rxs.at[0], rxr.at[0], x_peers[k],
            )

    merge_top(
        lambda i: runs2[i, 0:4, :], lambda i: runs2[i, 4:8, :], run_load(ctmp, 0), run_store(ctmp, 0), x_store,
        x_send,
    )
    xrecv[x_rows(x, 0, SENT), :] = xsend[x_rows(x, 0, SENT), :]
    take(xrecv.at[pl.ds(0, 3 * SENT)], rxr.at[0])

    def blocks(ref, base=0):
        return [ref[base + 8 * i : base + 8 * i + 8, :] for i in range(16)]

    def join(xs, ys):
        return [jnp.maximum(a, b) for a, b in zip(xs, ys)]

    lane = lax.broadcasted_iota(jnp.int32, (8, 128), 1)
    low = clean_rows(join(blocks(xrecv), blocks(xrecv, 128)))
    high = clean_rows(join(blocks(xrecv, 256), blocks(xrecv, 384)), True)
    up = ((lax.shift_right_logical(lane, 4) + 4 - y) & 3) >= 2
    merged = clean_rows(join(low, high), up)

    turned = jnp.concatenate(merged, axis=0).T
    for h in range(2):
        for y_ in range(4):
            for r8 in range(8):
                row = h * 64 + y_ * 16 + r8 * 2
                dsend[y_ * 16 + h * 8 + r8] = turned[row : row + 2, :]
    for k in (8, 7, 9, 6, 10, 5, 11, 4, 12, 3, 13, 2, 14, 1, 15, 0):
        for j in (2, 1, 3, 0):
            if (j, k) == (0, 0):
                continue
            n = j * 16 + SLOT[k]
            remote(
                dsend.at[((y + j) % 4) * 16 + SLOT[k]], drecv.at[n], rds.at[0], rdr.at[0],
                at(x, (y + j) % 4, (z + k) % 16, c),
            )
    drecv[0] = dsend[y * 16]
    take(drecv.at[1:64], rdr.at[0])
    for n in range(64):
        row_b[2 * n : 2 * n + 2, :] = drecv[n]
    row_a[...] = row_b[...].T
    merged = blocks(row_a)
    for distance in (64, 32, 16, 8, 4, 2):
        merged = join(merged, [pltpu.roll(v, 128 - distance, axis=1) for v in merged])
        up = (lane & (distance // 2)) != 0 if distance > 2 else None
        merged = clean_rows(merged, up)
    o_ref[...] = jnp.concatenate(merged, axis=0).T[0:2, 0:K]

    drain(zbuf.at[0:15], zs.at[0])
    for n in range(5):
        group, a2 = kinds[n][0], kinds[n][1]
        drain(group(a2).at[0:3], fs.at[n])
        drain(whole[n].at[0:3], ss.at[n])
    drain(v_vm.at[1], vs.at[0])
    drain(rows2, vs.at[1])
    drain(ids2, vs.at[2])
    drain(xrecv.at[pl.ds(0, 3 * SENT)], rxs.at[0])
    drain(dsend.at[0:63], rds.at[0])


def local(queries, probes, vectors, list_ids):
    vmem = pl.BlockSpec(memory_space=pltpu.VMEM)
    dma = pltpu.SemaphoreType.DMA
    return pl.pallas_call(
        kernel,
        out_shape=jax.ShapeDtypeStruct((2, K), F32),
        in_specs=[pl.BlockSpec(memory_space=pltpu.HBM)] * 5,
        out_specs=vmem,
        scratch_shapes=[
            pltpu.VMEM((2, 768), jnp.bfloat16),
            pltpu.VMEM((2, 16), jnp.int32),
            pltpu.VMEM((4, 128), jnp.int32),
            pltpu.VMEM((4, 128), jnp.int32),
            pltpu.VMEM((512,), jnp.int32),
            pltpu.VMEM((512,), jnp.int32),
            pltpu.SMEM((512,), jnp.int32),
            pltpu.SMEM((512,), jnp.int32),
            pltpu.VMEM((4096, 128), jnp.int32),
            pltpu.VMEM((16, 16, 128), jnp.bfloat16),
            pltpu.VMEM((2, 4, 4, 16, 384), jnp.bfloat16),
            pltpu.VMEM((2, 4, 4, 16, 384), jnp.bfloat16),
            pltpu.VMEM((4, 4, 16, 128), jnp.bfloat16),
            pltpu.VMEM((2, 512, 768), jnp.bfloat16),
            pltpu.VMEM((4096, 128), F32),
            pltpu.VMEM((32, 8, 128), jnp.int32),
            pltpu.VMEM((32, 8, 128), jnp.int32),
            pltpu.VMEM((256, 128), jnp.int32),
            pltpu.VMEM((512, 8, 128), F32),
            pltpu.VMEM((512, 8, 128), F32),
            pltpu.VMEM((128, 4, 128), F32),
            pltpu.VMEM((512, 128), F32),
            pltpu.VMEM((512, 128), F32),
            pltpu.VMEM((128, 128), F32),
            pltpu.VMEM((128, 128), F32),
            pltpu.VMEM((64, 2, 128), F32),
            pltpu.VMEM((64, 2, 128), F32),
            dma((6,)), dma((1,)), dma((3,)), dma((3,)), dma((1,)), dma((5,)), dma((5,)), dma((5, 3)), dma((5,)),
            dma((5, 3)), dma((1,)), dma((1,)), dma((1,)), dma((1,)),
        ],
        compiler_params=pltpu.CompilerParams(collective_id=0, has_side_effects=True),
    )(queries, probes, vectors, list_ids.reshape(4, 128), list_ids)


def solution(mesh):
    return jax.shard_map(
        local,
        mesh=mesh,
        in_specs=(
            P(("pb", "dev"), None),
            P(("pb", "dev"), None),
            P(("pb", "dev"), None),
            P(("pb", "dev")),
        ),
        out_specs=P(("pb", "dev"), None),
        check_vma=False,
    )
```

```python
import functools

import jax
import jax.numpy as jnp
from jax import lax
from jax.experimental import pallas as pl
from jax.experimental.pallas import tpu as pltpu
from jax.sharding import PartitionSpec as P

K = 100
SENT = 104
NEG = -1.0e30
MESH = pl.DeviceIdType.MESH
F32 = jnp.float32


SLOT = {k % 16: n for n, k in enumerate((0, 1, 2, 3, 4, -1, -2, -3, 5, 6, 7, 8, -4, -5, -6, -7))}


def exchange(a, b):
    return jnp.maximum(a, b), jnp.minimum(a, b)


def sort_desc(xs):
    xs, n, p = list(xs), len(xs), 1
    while p < n:
        k = p
        while k >= 1:
            for j in range(k % p, n - k, 2 * k):
                for i in range(min(k, n - j - k)):
                    if (i + j) // (2 * p) == (i + j + k) // (2 * p):
                        xs[i + j], xs[i + j + k] = exchange(xs[i + j], xs[i + j + k])
            k //= 2
        p *= 2
    return xs


def clean_desc(xs):
    xs, d = list(xs), len(xs) // 2
    while d >= 1:
        for i in range(len(xs)):
            if i & d == 0:
                xs[i], xs[i + d] = exchange(xs[i], xs[i + d])
        d //= 2
    return xs


def clean_rows(xs, up=None):
    def order(hi, lo):
        if up is None:
            return hi, lo
        if up is True:
            return lo, hi
        return jnp.where(up, lo, hi), jnp.where(up, hi, lo)

    xs = list(xs)
    for d in (8, 4, 2, 1):
        for i in range(16):
            if i & d == 0:
                xs[i], xs[i + d] = order(*exchange(xs[i], xs[i + d]))
    row = lax.broadcasted_iota(jnp.int32, (8, 128), 0)
    for d in (4, 2, 1):
        lower = (row & d) == 0
        if up is None:
            larger = lower
        elif up is True:
            larger = (row & d) != 0
        else:
            larger = lower != up
        for i in range(16):
            if d == 4:
                other = pltpu.roll(xs[i], 4, axis=0)
            else:
                other = jnp.where(lower, pltpu.roll(xs[i], 8 - d, axis=0), pltpu.roll(xs[i], d, axis=0))
            hi, lo = exchange(xs[i], other)
            xs[i] = jnp.where(larger, hi, lo)
    return xs


def merge_top(load_a, load_b, tmp_load, tmp_store, store, after=None):
    @pl.loop(0, 2)
    def _(g):
        for u in range(16):
            i = g * 16 + u
            m = [jnp.maximum(load_a(i + 32 * k), load_b(127 - i - 32 * k)) for k in range(4)]
            m[0], m[2] = exchange(m[0], m[2])
            m[1], m[3] = exchange(m[1], m[3])
            m[0], m[1] = exchange(m[0], m[1])
            m[2], m[3] = exchange(m[2], m[3])
            for k in range(4):
                tmp_store(i + 32 * k, m[k])

    def finish(k):
        xs = clean_desc([tmp_load(32 * k + i) for i in range(32)])
        for i in range(32):
            store(32 * k + i, xs[i])

    if after is None:
        pl.loop(0, 4)(finish)
    else:
        for k in range(4):
            finish(k)
            after(k)


def kernel(
    q_hbm, p_hbm, v_hbm, id_hbm, flat_hbm, o_ref,
    q_ref, p_ref, ids, ids2, flat, row_of, rows1, rows2, bit_of, zbuf, ga, gb, gc, v_vm, prod, words, words2, codes, runs, runs2, ctmp,
    xsend, xrecv, row_a, row_b, dsend, drecv,
    in_sem, done, vs, vr, zs, zr, fs, fr, ss, sr, rxs, rxr, rds, rdr,
):
    pb, dev = lax.axis_index("pb"), lax.axis_index("dev")
    x, ylo, c = pb // 4, (pb // 2) % 2, pb % 2
    z, yhi = dev // 2, dev % 2
    y = yhi * 2 + ylo

    def at(x_, y_, z_, c_):
        return {"pb": x_ * 4 + (y_ % 2) * 2 + c_, "dev": z_ * 2 + y_ // 2}

    z_peers = {k: at(x, y, (z + k) % 16, c) for k in range(1, 16)}
    y_peers = [at(x, (y + k) % 4, z, c) for k in range(1, 4)]
    x_peers = [at((x + k) % 4, y, z, c) for k in range(1, 4)]
    partner = at(x, y, z, 1 - c)

    barrier = pltpu.get_barrier_semaphore()
    near = (4, 12, 3, 13, 2, 14, 1, 15)
    everyone = [z_peers[k] for k in near] + y_peers + x_peers + [partner]
    for peer in everyone:
        pl.semaphore_signal(barrier, inc=1, device_id=peer, device_id_type=MESH)

    fetch = [
        pltpu.make_async_copy(src, dst, in_sem.at[n])
        for n, (src, dst) in enumerate(
            ((q_hbm, q_ref), (p_hbm, p_ref), (id_hbm, ids), (v_hbm, v_vm.at[0]), (flat_hbm, flat))
        )
    ]
    for copy in fetch:
        copy.start()
    for s in range(4):
        pad = s * 128 + (0 if s % 2 else SENT)
        xrecv[pad : pad + 128 - SENT, :] = jnp.full((128 - SENT, 128), NEG, F32)
    fetch[0].wait()
    fetch[1].wait()

    zbuf[0, 12:16, :] = jnp.zeros((4, 128), jnp.bfloat16)
    for i in range(6):
        zbuf[0, 2 * i : 2 * i + 2, :] = q_ref[:, 128 * i : 128 * i + 128]
    lists = p_ref[...]
    zbuf[0, 12:14, 0:16] = lax.shift_right_logical(lists, 5).astype(F32).astype(jnp.bfloat16)
    zbuf[0, 12:14, 16:32] = (lists & 31).astype(F32).astype(jnp.bfloat16)
    pl.semaphore_wait(barrier, len(everyone))

    def remote(src, dst, send, recv, peer):
        copy = pltpu.make_async_remote_copy(
            src_ref=src, dst_ref=dst, send_sem=send, recv_sem=recv,
            device_id=peer, device_id_type=MESH,
        )
        copy.start()
        return copy

    def take(ref, recv):
        pltpu.make_async_remote_copy(
            src_ref=ref, dst_ref=ref, send_sem=done.at[0], recv_sem=recv,
            device_id=partner, device_id_type=MESH,
        ).wait_recv()

    def drain(ref, send):
        pltpu.make_async_remote_copy(
            src_ref=ref, dst_ref=ref, send_sem=send, recv_sem=done.at[0],
            device_id=partner, device_id_type=MESH,
        ).wait_send()

    def z_send(block, k, n):
        remote(zbuf.at[SLOT[block % 16]], zbuf.at[SLOT[(block - k) % 16]], zs.at[0], zr.at[n], z_peers[k])

    for k in near:
        z_send(0, k, min(k, 16 - k))
    remote(v_hbm, v_vm.at[1], vs.at[0], vr.at[0], partner)
    fetch[2].wait()
    fetch[4].wait()
    row_of[...] = lax.shift_right_logical(flat[...], 5)
    table = pltpu.make_async_copy(row_of, rows1, in_sem.at[5])
    table.start()
    remote(row_of, rows2, vs.at[1], vr.at[1], partner)
    remote(ids, ids2, vs.at[2], vr.at[2], partner)
    r = lax.broadcasted_iota(jnp.int32, (112, 128), 0)
    k_ = lax.broadcasted_iota(jnp.int32, (112, 128), 1)
    pick = k_ == lax.shift_right_logical(r & 15, 1) * 16 + lax.shift_right_logical(r, 4) * 2 + (r & 1)
    pick = jnp.where(pick, 1.0, 0.0).astype(jnp.bfloat16)

    def place(h):
        rows = jnp.dot(
            pick, zbuf[8 * h : 8 * h + 8].reshape(128, 128), preferred_element_type=F32
        )
        for i in range(3):
            ga[h, x, y, :, 128 * i : 128 * i + 128] = rows[16 * i : 16 * i + 16, :].astype(jnp.bfloat16)
            gb[h, y, x, :, 128 * i : 128 * i + 128] = rows[16 * i + 48 : 16 * i + 64, :].astype(jnp.bfloat16)
        return rows[96:112, :]

    kinds = [
        (lambda a2, h=h, g=g: g.at[h, a2], *axes)
        for h in range(2)
        for g, axes in ((ga, (x, y, y_peers, x_peers)), (gb, (y, x, x_peers, y_peers)))
    ]
    whole = [ga.at[0], gb.at[0], ga.at[1], gb.at[1], gc]
    kinds.append((lambda a2: gc.at[a2], x, y, y_peers, x_peers))

    def send_first(n):
        group, a2, a1, peers, _ = kinds[n]
        ref = group(a2).at[a1]
        for k in (1, 0, 2):
            remote(ref, ref, fs.at[n], fr.at[n, k], peers[k])

    def send_second(n, b):
        group, a2, a1, _, peers = kinds[n]
        ref = group(a2).at[(a1 + 4 - b) % 4]
        for k in (1, 0, 2):
            remote(ref, ref, ss.at[n], sr.at[n, k], peers[k])

    def pass_first(which):
        for b in (1, 3, 2):
            for n in which:
                take(kinds[n][0](kinds[n][1]).at[0], fr.at[n, b - 1])
                send_second(n, b)

    def pass_second(which):
        for b in (1, 3, 2):
            for n in which:
                take(kinds[n][0](kinds[n][1]), sr.at[n, b - 1])

    def start(which):
        for n in which:
            send_first(n)
        for n in which:
            send_second(n, 0)

    for j in (1, 2, 3, 4):
        take(zbuf.at[0:2], zr.at[j])
        z_send(-j, 4, 0)
        if j < 4:
            z_send(j, 12, 0)
    near_codes = place(0)
    start((0, 1))

    take(ids2, vr.at[2])
    for part in range(4):
        for s, ref in enumerate((ids, ids2)):
            column = jnp.broadcast_to(ref[part : part + 1, :], (128, 128)).T
            bit = jnp.left_shift(jnp.int32(1), column & 31)
            for t in range(4):
                bit_of[pl.ds(part * 1024 + 4 * s + t, 128, stride=8), :] = bit

    take(zbuf.at[0:7], zr.at[0])
    far_codes = place(1)
    gc[x, y] = (near_codes + pltpu.roll(far_codes, 32, axis=1)).astype(jnp.bfloat16)
    start((4, 2, 3))
    pass_first((0, 1))
    pass_first((4, 2, 3))
    pass_second((0, 1))
    fetch[3].wait()
    table.wait()
    take(v_vm.at[1], vr.at[0])
    take(rows2, vr.at[1])

    def score(h):
        block = jnp.concatenate(
            [
                jnp.concatenate([ga[h, s].reshape(64, 384), gb[h, :, s].reshape(64, 384)], axis=1)
                for s in range(4)
            ],
            axis=0,
        )

        @pl.loop(0, 2)
        def _(core):
            scores = lax.dot_general(
                v_vm[core], block, (((1,), (1,)), ((), ())), preferred_element_type=F32
            )
            for s in range(4):
                part = scores[:, 128 * (s // 2) : 128 * (s // 2) + 128]
                if s % 2 != h:
                    part = pltpu.roll(part, 64, axis=1)
                for j in range(64):
                    row = pl.multiple_of(j * 64 + (core * 4 + s) * 8, 8)
                    prod[pl.ds(row, 8), 64 * h : 64 * h + 64] = part[
                        8 * j : 8 * j + 8, 64 * h : 64 * h + 64
                    ]

    score(0)
    pass_second((4,))
    for s in range(4):
        turned = gc[s].reshape(64, 128).astype(F32).T.astype(jnp.int32)
        turned = jnp.concatenate([turned[0:32, :], turned[32:64, :]], axis=1)
        codes[32 * s : 32 * s + 32, :] = turned
        codes[32 * s + 128 : 32 * s + 160, :] = turned
    high = [codes[pl.ds(p, 8, stride=32), :] for p in range(16)]
    bits = [jnp.left_shift(jnp.int32(1), codes[pl.ds(16 + p, 8, stride=32), :]) for p in range(16)]
    own = lax.broadcasted_iota(jnp.int32, (8, 128), 0) < 4

    @pl.loop(0, 8)
    def _(a4):
        for a in range(4):
            terms = [jnp.where(high[p] == a4 * 4 + a, bits[p], 0) for p in range(16)]
            while len(terms) > 1:
                terms = [terms[i] | terms[i + 1] for i in range(0, len(terms), 2)]
            words[a4 * 4 + a] = jnp.where(own, terms[0], 0)
            words2[a4 * 4 + a] = jnp.where(own, 0, terms[0])

    pass_second((2, 3))
    score(1)

    @pl.loop(0, 16)
    def _(g):
        xs = []
        for i in range(32):
            value = prod[pl.ds(g * 256 + (i // 8) * 64 + i % 8, 8, stride=8), :]
            word = words[rows1[g * 32 + i]] | words2[rows2[g * 32 + i]]
            found = word & bit_of[pl.ds(pl.multiple_of(g * 256 + i * 8, 8), 8), :]
            xs.append(jnp.where(found != 0, value, NEG))
        xs = sort_desc(xs)
        for i in range(32):
            runs[g * 32 + i] = xs[i]

    @pl.loop(0, 8)
    def _(g):
        base = g * 64
        for side, op in ((0, jnp.maximum), (1, jnp.minimum)):
            xs = [op(runs[base + i], runs[base + 63 - i]) for i in range(32)]
            xs = clean_desc(xs)
            for i in range(32):
                runs2[base + 32 * side + i] = xs[i]

    @pl.loop(0, 4)
    def _(g):
        base = g * 128
        for i in range(32):
            a, b = runs2[base + i], runs2[base + 127 - i]
            a2, b2 = runs2[base + 32 + i], runs2[base + 95 - i]
            h1, l1 = exchange(a, b)
            h2, l2 = exchange(a2, b2)
            h1, h2 = exchange(h1, h2)
            l1, l2 = exchange(l1, l2)
            runs[base + i], runs[base + 32 + i] = h1, h2
            runs[base + 64 + i], runs[base + 96 + i] = l1, l2

    @pl.loop(0, 16)
    def _(g):
        xs = clean_desc([runs[g * 32 + i] for i in range(32)])
        for i in range(32):
            runs2[g * 32 + i] = xs[i]

    def run_store(ref, base):
        def put(i, value):
            ref[base + i] = value
        return put

    def run_load(ref, base):
        return lambda i: ref[base + i]

    for g in range(2):
        merge_top(
            run_load(runs2, 256 * g), run_load(runs2, 256 * g + 128),
            run_load(runs, 256 * g), run_store(runs, 256 * g), run_store(runs2, 256 * g),
        )

    merge_top(
        run_load(runs2, 0), run_load(runs2, 256), run_load(runs, 0), run_store(runs, 0), run_store(runs2, 0)
    )

    def x_store(i, value):
        xsend[pl.ds(i + (x & 1) * (127 - 2 * i), 4, stride=128), :] = value

    def x_rows(s, start, size):
        ascending = 128 - size - start
        return pl.ds(pl.multiple_of(s * 128 + start + (x & 1) * (ascending - start), 8), size)

    def x_send(q):
        start, size = 32 * q, min(32, SENT - 32 * q)
        for k in (1, 0, 2):
            remote(
                xsend.at[x_rows((x + k + 1) % 4, start, size)], xrecv.at[x_rows(x, start, size)],
                rxs.at[0], rxr.at[0], x_peers[k],
            )

    merge_top(
        lambda i: runs2[i, 0:4, :], lambda i: runs2[i, 4:8, :], run_load(ctmp, 0), run_store(ctmp, 0), x_store,
        x_send,
    )
    xrecv[x_rows(x, 0, SENT), :] = xsend[x_rows(x, 0, SENT), :]
    take(xrecv.at[pl.ds(0, 3 * SENT)], rxr.at[0])

    def blocks(ref, base=0):
        return [ref[base + 8 * i : base + 8 * i + 8, :] for i in range(16)]

    def join(xs, ys):
        return [jnp.maximum(a, b) for a, b in zip(xs, ys)]

    lane = lax.broadcasted_iota(jnp.int32, (8, 128), 1)
    low = clean_rows(join(blocks(xrecv), blocks(xrecv, 128)))
    high = clean_rows(join(blocks(xrecv, 256), blocks(xrecv, 384)), True)
    up = ((lax.shift_right_logical(lane, 4) + 4 - y) & 3) >= 2
    merged = clean_rows(join(low, high), up)

    turned = jnp.concatenate(merged, axis=0).T
    for h in range(2):
        for y_ in range(4):
            for r8 in range(8):
                row = h * 64 + y_ * 16 + r8 * 2
                dsend[y_ * 16 + h * 8 + r8] = turned[row : row + 2, :]
    for k in (8, 7, 9, 6, 10, 5, 11, 4, 12, 3, 13, 2, 14, 1, 15, 0):
        for j in (2, 1, 3, 0):
            if (j, k) == (0, 0):
                continue
            n = j * 16 + SLOT[k]
            remote(
                dsend.at[((y + j) % 4) * 16 + SLOT[k]], drecv.at[n], rds.at[0], rdr.at[0],
                at(x, (y + j) % 4, (z + k) % 16, c),
            )
    drecv[0] = dsend[y * 16]
    take(drecv.at[1:64], rdr.at[0])
    for n in range(64):
        row_b[2 * n : 2 * n + 2, :] = drecv[n]
    row_a[...] = row_b[...].T
    merged = blocks(row_a)
    for distance in (64, 32, 16, 8, 4, 2):
        merged = join(merged, [pltpu.roll(v, 128 - distance, axis=1) for v in merged])
        up = (lane & (distance // 2)) != 0 if distance > 2 else None
        merged = clean_rows(merged, up)
    o_ref[...] = jnp.concatenate(merged, axis=0).T[0:2, 0:K]

    drain(zbuf.at[0:15], zs.at[0])
    for n in range(5):
        group, a2 = kinds[n][0], kinds[n][1]
        drain(group(a2).at[0:3], fs.at[n])
        drain(whole[n].at[0:3], ss.at[n])
    drain(v_vm.at[1], vs.at[0])
    drain(rows2, vs.at[1])
    drain(ids2, vs.at[2])
    drain(xrecv.at[pl.ds(0, 3 * SENT)], rxs.at[0])
    drain(dsend.at[0:63], rds.at[0])


def local(queries, probes, vectors, list_ids):
    vmem = pl.BlockSpec(memory_space=pltpu.VMEM)
    dma = pltpu.SemaphoreType.DMA
    return pl.pallas_call(
        kernel,
        out_shape=jax.ShapeDtypeStruct((2, K), F32),
        in_specs=[pl.BlockSpec(memory_space=pltpu.HBM)] * 5,
        out_specs=vmem,
        scratch_shapes=[
            pltpu.VMEM((2, 768), jnp.bfloat16),
            pltpu.VMEM((2, 16), jnp.int32),
            pltpu.VMEM((4, 128), jnp.int32),
            pltpu.VMEM((4, 128), jnp.int32),
            pltpu.VMEM((512,), jnp.int32),
            pltpu.VMEM((512,), jnp.int32),
            pltpu.SMEM((512,), jnp.int32),
            pltpu.SMEM((512,), jnp.int32),
            pltpu.VMEM((4096, 128), jnp.int32),
            pltpu.VMEM((16, 16, 128), jnp.bfloat16),
            pltpu.VMEM((2, 4, 4, 16, 384), jnp.bfloat16),
            pltpu.VMEM((2, 4, 4, 16, 384), jnp.bfloat16),
            pltpu.VMEM((4, 4, 16, 128), jnp.bfloat16),
            pltpu.VMEM((2, 512, 768), jnp.bfloat16),
            pltpu.VMEM((4096, 128), F32),
            pltpu.VMEM((32, 8, 128), jnp.int32),
            pltpu.VMEM((32, 8, 128), jnp.int32),
            pltpu.VMEM((256, 128), jnp.int32),
            pltpu.VMEM((512, 8, 128), F32),
            pltpu.VMEM((512, 8, 128), F32),
            pltpu.VMEM((128, 4, 128), F32),
            pltpu.VMEM((512, 128), F32),
            pltpu.VMEM((512, 128), F32),
            pltpu.VMEM((128, 128), F32),
            pltpu.VMEM((128, 128), F32),
            pltpu.VMEM((64, 2, 128), F32),
            pltpu.VMEM((64, 2, 128), F32),
            dma((6,)), dma((1,)), dma((3,)), dma((3,)), dma((1,)), dma((5,)), dma((5,)), dma((5, 3)), dma((5,)),
            dma((5, 3)), dma((1,)), dma((1,)), dma((1,)), dma((1,)),
        ],
        compiler_params=pltpu.CompilerParams(collective_id=0, has_side_effects=True, vmem_limit_bytes=56550000),
    )(queries, probes, vectors, list_ids.reshape(4, 128), list_ids)


def solution(mesh):
    return jax.shard_map(
        local,
        mesh=mesh,
        in_specs=(
            P(("pb", "dev"), None),
            P(("pb", "dev"), None),
            P(("pb", "dev"), None),
            P(("pb", "dev")),
        ),
        out_specs=P(("pb", "dev"), None),
        check_vma=False,
    )
```

```python
import functools

import jax
import jax.numpy as jnp
from jax import lax
from jax.experimental import pallas as pl
from jax.experimental.pallas import tpu as pltpu
from jax.sharding import PartitionSpec as P

K = 100
SENT = 104
NEG = -1.0e30
MESH = pl.DeviceIdType.MESH
F32 = jnp.float32


SLOT = {k % 16: n for n, k in enumerate((0, 1, 2, 3, 4, -1, -2, -3, 5, 6, 7, 8, -4, -5, -6, -7))}


def exchange(a, b):
    return jnp.maximum(a, b), jnp.minimum(a, b)


def sort_desc(xs):
    xs, n, p = list(xs), len(xs), 1
    while p < n:
        k = p
        while k >= 1:
            for j in range(k % p, n - k, 2 * k):
                for i in range(min(k, n - j - k)):
                    if (i + j) // (2 * p) == (i + j + k) // (2 * p):
                        xs[i + j], xs[i + j + k] = exchange(xs[i + j], xs[i + j + k])
            k //= 2
        p *= 2
    return xs


def clean_desc(xs):
    xs, d = list(xs), len(xs) // 2
    while d >= 1:
        for i in range(len(xs)):
            if i & d == 0:
                xs[i], xs[i + d] = exchange(xs[i], xs[i + d])
        d //= 2
    return xs


def clean_rows(xs, up=None):
    def order(hi, lo):
        if up is None:
            return hi, lo
        if up is True:
            return lo, hi
        return jnp.where(up, lo, hi), jnp.where(up, hi, lo)

    xs = list(xs)
    for d in (8, 4, 2, 1):
        for i in range(16):
            if i & d == 0:
                xs[i], xs[i + d] = order(*exchange(xs[i], xs[i + d]))
    row = lax.broadcasted_iota(jnp.int32, (8, 128), 0)
    for d in (4, 2, 1):
        lower = (row & d) == 0
        if up is None:
            larger = lower
        elif up is True:
            larger = (row & d) != 0
        else:
            larger = lower != up
        for i in range(16):
            if d == 4:
                other = pltpu.roll(xs[i], 4, axis=0)
            else:
                other = jnp.where(lower, pltpu.roll(xs[i], 8 - d, axis=0), pltpu.roll(xs[i], d, axis=0))
            hi, lo = exchange(xs[i], other)
            xs[i] = jnp.where(larger, hi, lo)
    return xs


def merge_top(load_a, load_b, tmp_load, tmp_store, store, after=None):
    @pl.loop(0, 2)
    def _(g):
        for u in range(16):
            i = g * 16 + u
            m = [jnp.maximum(load_a(i + 32 * k), load_b(127 - i - 32 * k)) for k in range(4)]
            m[0], m[2] = exchange(m[0], m[2])
            m[1], m[3] = exchange(m[1], m[3])
            m[0], m[1] = exchange(m[0], m[1])
            m[2], m[3] = exchange(m[2], m[3])
            for k in range(4):
                tmp_store(i + 32 * k, m[k])

    def finish(k):
        xs = clean_desc([tmp_load(32 * k + i) for i in range(32)])
        for i in range(32):
            store(32 * k + i, xs[i])

    if after is None:
        @pl.loop(0, 2)
        def _(pair):
            finish(pair * 2)
            finish(pair * 2 + 1)
    else:
        for k in range(4):
            finish(k)
            after(k)


def kernel(
    q_hbm, p_hbm, v_hbm, id_hbm, flat_hbm, o_ref,
    q_ref, p_ref, ids, ids2, flat, row_of, rows1, rows2, bit_of, zbuf, ga, gb, gc, v_vm, prod, words, words2, codes, runs, runs2, ctmp,
    xsend, xrecv, row_a, row_b, dsend, drecv,
    in_sem, done, vs, vr, zs, zr, fs, fr, ss, sr, rxs, rxr, rds, rdr,
):
    pb, dev = lax.axis_index("pb"), lax.axis_index("dev")
    x, ylo, c = pb // 4, (pb // 2) % 2, pb % 2
    z, yhi = dev // 2, dev % 2
    y = yhi * 2 + ylo

    def at(x_, y_, z_, c_):
        return {"pb": x_ * 4 + (y_ % 2) * 2 + c_, "dev": z_ * 2 + y_ // 2}

    z_peers = {k: at(x, y, (z + k) % 16, c) for k in range(1, 16)}
    y_peers = [at(x, (y + k) % 4, z, c) for k in range(1, 4)]
    x_peers = [at((x + k) % 4, y, z, c) for k in range(1, 4)]
    partner = at(x, y, z, 1 - c)

    barrier = pltpu.get_barrier_semaphore()
    near = (4, 12, 3, 13, 2, 14, 1, 15)
    everyone = [z_peers[k] for k in near] + y_peers + x_peers + [partner]
    for peer in everyone:
        pl.semaphore_signal(barrier, inc=1, device_id=peer, device_id_type=MESH)

    fetch = [
        pltpu.make_async_copy(src, dst, in_sem.at[n])
        for n, (src, dst) in enumerate(
            ((q_hbm, q_ref), (p_hbm, p_ref), (id_hbm, ids), (v_hbm, v_vm.at[0]), (flat_hbm, flat))
        )
    ]
    for copy in fetch:
        copy.start()
    for s in range(4):
        pad = s * 128 + (0 if s % 2 else SENT)
        xrecv[pad : pad + 128 - SENT, :] = jnp.full((128 - SENT, 128), NEG, F32)
    fetch[0].wait()
    fetch[1].wait()

    zbuf[0, 12:16, :] = jnp.zeros((4, 128), jnp.bfloat16)
    for i in range(6):
        zbuf[0, 2 * i : 2 * i + 2, :] = q_ref[:, 128 * i : 128 * i + 128]
    lists = p_ref[...]
    zbuf[0, 12:14, 0:16] = lax.shift_right_logical(lists, 5).astype(F32).astype(jnp.bfloat16)
    zbuf[0, 12:14, 16:32] = (lists & 31).astype(F32).astype(jnp.bfloat16)
    pl.semaphore_wait(barrier, len(everyone))

    def remote(src, dst, send, recv, peer):
        copy = pltpu.make_async_remote_copy(
            src_ref=src, dst_ref=dst, send_sem=send, recv_sem=recv,
            device_id=peer, device_id_type=MESH,
        )
        copy.start()
        return copy

    def take(ref, recv):
        pltpu.make_async_remote_copy(
            src_ref=ref, dst_ref=ref, send_sem=done.at[0], recv_sem=recv,
            device_id=partner, device_id_type=MESH,
        ).wait_recv()

    def drain(ref, send):
        pltpu.make_async_remote_copy(
            src_ref=ref, dst_ref=ref, send_sem=send, recv_sem=done.at[0],
            device_id=partner, device_id_type=MESH,
        ).wait_send()

    def z_send(block, k, n):
        remote(zbuf.at[SLOT[block % 16]], zbuf.at[SLOT[(block - k) % 16]], zs.at[0], zr.at[n], z_peers[k])

    for k in near:
        z_send(0, k, min(k, 16 - k))
    remote(v_hbm, v_vm.at[1], vs.at[0], vr.at[0], partner)
    fetch[2].wait()
    fetch[4].wait()
    row_of[...] = lax.shift_right_logical(flat[...], 5)
    table = pltpu.make_async_copy(row_of, rows1, in_sem.at[5])
    table.start()
    remote(row_of, rows2, vs.at[1], vr.at[1], partner)
    remote(ids, ids2, vs.at[2], vr.at[2], partner)
    r = lax.broadcasted_iota(jnp.int32, (112, 128), 0)
    k_ = lax.broadcasted_iota(jnp.int32, (112, 128), 1)
    pick = k_ == lax.shift_right_logical(r & 15, 1) * 16 + lax.shift_right_logical(r, 4) * 2 + (r & 1)
    pick = jnp.where(pick, 1.0, 0.0).astype(jnp.bfloat16)

    def place(h):
        rows = jnp.dot(
            pick, zbuf[8 * h : 8 * h + 8].reshape(128, 128), preferred_element_type=F32
        )
        for i in range(3):
            ga[h, x, y, :, 128 * i : 128 * i + 128] = rows[16 * i : 16 * i + 16, :].astype(jnp.bfloat16)
            gb[h, y, x, :, 128 * i : 128 * i + 128] = rows[16 * i + 48 : 16 * i + 64, :].astype(jnp.bfloat16)
        return rows[96:112, :]

    kinds = [
        (lambda a2, h=h, g=g: g.at[h, a2], *axes)
        for h in range(2)
        for g, axes in ((ga, (x, y, y_peers, x_peers)), (gb, (y, x, x_peers, y_peers)))
    ]
    whole = [ga.at[0], gb.at[0], ga.at[1], gb.at[1], gc]
    kinds.append((lambda a2: gc.at[a2], x, y, y_peers, x_peers))

    def send_first(n):
        group, a2, a1, peers, _ = kinds[n]
        ref = group(a2).at[a1]
        for k in (1, 0, 2):
            remote(ref, ref, fs.at[n], fr.at[n, k], peers[k])

    def send_second(n, b):
        group, a2, a1, _, peers = kinds[n]
        ref = group(a2).at[(a1 + 4 - b) % 4]
        for k in (1, 0, 2):
            remote(ref, ref, ss.at[n], sr.at[n, k], peers[k])

    def pass_first(which):
        for b in (1, 3, 2):
            for n in which:
                take(kinds[n][0](kinds[n][1]).at[0], fr.at[n, b - 1])
                send_second(n, b)

    def pass_second(which):
        for b in (1, 3, 2):
            for n in which:
                take(kinds[n][0](kinds[n][1]), sr.at[n, b - 1])

    def start(which):
        for n in which:
            send_first(n)
        for n in which:
            send_second(n, 0)

    for j in (1, 2, 3, 4):
        take(zbuf.at[0:2], zr.at[j])
        z_send(-j, 4, 0)
        if j < 4:
            z_send(j, 12, 0)
    near_codes = place(0)
    start((0, 1))

    take(ids2, vr.at[2])
    for part in range(4):
        for s, ref in enumerate((ids, ids2)):
            column = jnp.broadcast_to(ref[part : part + 1, :], (128, 128)).T
            bit = jnp.left_shift(jnp.int32(1), column & 31)
            for t in range(4):
                bit_of[pl.ds(part * 1024 + 4 * s + t, 128, stride=8), :] = bit

    take(zbuf.at[0:7], zr.at[0])
    far_codes = place(1)
    gc[x, y] = (near_codes + pltpu.roll(far_codes, 32, axis=1)).astype(jnp.bfloat16)
    start((4, 2, 3))
    pass_first((0, 1))
    pass_first((4, 2, 3))
    pass_second((0, 1))
    fetch[3].wait()
    table.wait()
    take(v_vm.at[1], vr.at[0])
    take(rows2, vr.at[1])

    def score(h):
        block = jnp.concatenate(
            [
                jnp.concatenate([ga[h, s].reshape(64, 384), gb[h, :, s].reshape(64, 384)], axis=1)
                for s in range(4)
            ],
            axis=0,
        )

        @pl.loop(0, 2)
        def _(core):
            scores = lax.dot_general(
                v_vm[core], block, (((1,), (1,)), ((), ())), preferred_element_type=F32
            )
            for s in range(4):
                part = scores[:, 128 * (s // 2) : 128 * (s // 2) + 128]
                if s % 2 != h:
                    part = pltpu.roll(part, 64, axis=1)
                for j in range(64):
                    row = pl.multiple_of(j * 64 + (core * 4 + s) * 8, 8)
                    prod[pl.ds(row, 8), 64 * h : 64 * h + 64] = part[
                        8 * j : 8 * j + 8, 64 * h : 64 * h + 64
                    ]

    score(0)
    pass_second((4,))
    for s in range(4):
        turned = gc[s].reshape(64, 128).astype(F32).T.astype(jnp.int32)
        turned = jnp.concatenate([turned[0:32, :], turned[32:64, :]], axis=1)
        codes[32 * s : 32 * s + 32, :] = turned
        codes[32 * s + 128 : 32 * s + 160, :] = turned
    high = [codes[pl.ds(p, 8, stride=32), :] for p in range(16)]
    bits = [jnp.left_shift(jnp.int32(1), codes[pl.ds(16 + p, 8, stride=32), :]) for p in range(16)]
    own = lax.broadcasted_iota(jnp.int32, (8, 128), 0) < 4

    @pl.loop(0, 8)
    def _(a4):
        for a in range(4):
            terms = [jnp.where(high[p] == a4 * 4 + a, bits[p], 0) for p in range(16)]
            while len(terms) > 1:
                terms = [terms[i] | terms[i + 1] for i in range(0, len(terms), 2)]
            words[a4 * 4 + a] = jnp.where(own, terms[0], 0)
            words2[a4 * 4 + a] = jnp.where(own, 0, terms[0])

    pass_second((2, 3))
    score(1)

    @pl.loop(0, 16)
    def _(g):
        xs = []
        for i in range(32):
            value = prod[pl.ds(g * 256 + (i // 8) * 64 + i % 8, 8, stride=8), :]
            word = words[rows1[g * 32 + i]] | words2[rows2[g * 32 + i]]
            found = word & bit_of[pl.ds(pl.multiple_of(g * 256 + i * 8, 8), 8), :]
            xs.append(jnp.where(found != 0, value, NEG))
        xs = sort_desc(xs)
        for i in range(32):
            runs[g * 32 + i] = xs[i]

    @pl.loop(0, 8)
    def _(g):
        base = g * 64
        for side, op in ((0, jnp.maximum), (1, jnp.minimum)):
            xs = [op(runs[base + i], runs[base + 63 - i]) for i in range(32)]
            xs = clean_desc(xs)
            for i in range(32):
                runs2[base + 32 * side + i] = xs[i]

    @pl.loop(0, 4)
    def _(g):
        base = g * 128
        for i in range(32):
            a, b = runs2[base + i], runs2[base + 127 - i]
            a2, b2 = runs2[base + 32 + i], runs2[base + 95 - i]
            h1, l1 = exchange(a, b)
            h2, l2 = exchange(a2, b2)
            h1, h2 = exchange(h1, h2)
            l1, l2 = exchange(l1, l2)
            runs[base + i], runs[base + 32 + i] = h1, h2
            runs[base + 64 + i], runs[base + 96 + i] = l1, l2

    @pl.loop(0, 8)
    def _(pair):
        for g in (pair * 2, pair * 2 + 1):
            xs = clean_desc([runs[g * 32 + i] for i in range(32)])
            for i in range(32):
                runs2[g * 32 + i] = xs[i]

    def run_store(ref, base):
        def put(i, value):
            ref[base + i] = value
        return put

    def run_load(ref, base):
        return lambda i: ref[base + i]

    for g in range(2):
        merge_top(
            run_load(runs2, 256 * g), run_load(runs2, 256 * g + 128),
            run_load(runs, 256 * g), run_store(runs, 256 * g), run_store(runs2, 256 * g),
        )

    merge_top(
        run_load(runs2, 0), run_load(runs2, 256), run_load(runs, 0), run_store(runs, 0), run_store(runs2, 0)
    )

    def x_store(i, value):
        xsend[pl.ds(i + (x & 1) * (127 - 2 * i), 4, stride=128), :] = value

    def x_rows(s, start, size):
        ascending = 128 - size - start
        return pl.ds(pl.multiple_of(s * 128 + start + (x & 1) * (ascending - start), 8), size)

    def x_send(q):
        start, size = 32 * q, min(32, SENT - 32 * q)
        for k in (1, 0, 2):
            remote(
                xsend.at[x_rows((x + k + 1) % 4, start, size)], xrecv.at[x_rows(x, start, size)],
                rxs.at[0], rxr.at[0], x_peers[k],
            )

    merge_top(
        lambda i: runs2[i, 0:4, :], lambda i: runs2[i, 4:8, :], run_load(ctmp, 0), run_store(ctmp, 0), x_store,
        x_send,
    )
    xrecv[x_rows(x, 0, SENT), :] = xsend[x_rows(x, 0, SENT), :]
    take(xrecv.at[pl.ds(0, 3 * SENT)], rxr.at[0])

    def blocks(ref, base=0):
        return [ref[base + 8 * i : base + 8 * i + 8, :] for i in range(16)]

    def join(xs, ys):
        return [jnp.maximum(a, b) for a, b in zip(xs, ys)]

    lane = lax.broadcasted_iota(jnp.int32, (8, 128), 1)
    low = clean_rows(join(blocks(xrecv), blocks(xrecv, 128)))
    high = clean_rows(join(blocks(xrecv, 256), blocks(xrecv, 384)), True)
    up = ((lax.shift_right_logical(lane, 4) + 4 - y) & 3) >= 2
    merged = clean_rows(join(low, high), up)

    turned = jnp.concatenate(merged, axis=0).T
    for h in range(2):
        for y_ in range(4):
            for r8 in range(8):
                row = h * 64 + y_ * 16 + r8 * 2
                dsend[y_ * 16 + h * 8 + r8] = turned[row : row + 2, :]
    for k in (8, 7, 9, 6, 10, 5, 11, 4, 12, 3, 13, 2, 14, 1, 15, 0):
        for j in (2, 1, 3, 0):
            if (j, k) == (0, 0):
                continue
            n = j * 16 + SLOT[k]
            remote(
                dsend.at[((y + j) % 4) * 16 + SLOT[k]], drecv.at[n], rds.at[0], rdr.at[0],
                at(x, (y + j) % 4, (z + k) % 16, c),
            )
    drecv[0] = dsend[y * 16]
    take(drecv.at[1:64], rdr.at[0])
    for n in range(64):
        row_b[2 * n : 2 * n + 2, :] = drecv[n]
    row_a[...] = row_b[...].T
    merged = blocks(row_a)
    for distance in (64, 32, 16, 8, 4, 2):
        merged = join(merged, [pltpu.roll(v, 128 - distance, axis=1) for v in merged])
        up = (lane & (distance // 2)) != 0 if distance > 2 else None
        merged = clean_rows(merged, up)
    o_ref[...] = jnp.concatenate(merged, axis=0).T[0:2, 0:K]

    drain(zbuf.at[0:15], zs.at[0])
    for n in range(5):
        group, a2 = kinds[n][0], kinds[n][1]
        drain(group(a2).at[0:3], fs.at[n])
        drain(whole[n].at[0:3], ss.at[n])
    drain(v_vm.at[1], vs.at[0])
    drain(rows2, vs.at[1])
    drain(ids2, vs.at[2])
    drain(xrecv.at[pl.ds(0, 3 * SENT)], rxs.at[0])
    drain(dsend.at[0:63], rds.at[0])


def local(queries, probes, vectors, list_ids):
    vmem = pl.BlockSpec(memory_space=pltpu.VMEM)
    dma = pltpu.SemaphoreType.DMA
    return pl.pallas_call(
        kernel,
        out_shape=jax.ShapeDtypeStruct((2, K), F32),
        in_specs=[pl.BlockSpec(memory_space=pltpu.HBM)] * 5,
        out_specs=vmem,
        scratch_shapes=[
            pltpu.VMEM((2, 768), jnp.bfloat16),
            pltpu.VMEM((2, 16), jnp.int32),
            pltpu.VMEM((4, 128), jnp.int32),
            pltpu.VMEM((4, 128), jnp.int32),
            pltpu.VMEM((512,), jnp.int32),
            pltpu.VMEM((512,), jnp.int32),
            pltpu.SMEM((512,), jnp.int32),
            pltpu.SMEM((512,), jnp.int32),
            pltpu.VMEM((4096, 128), jnp.int32),
            pltpu.VMEM((16, 16, 128), jnp.bfloat16),
            pltpu.VMEM((2, 4, 4, 16, 384), jnp.bfloat16),
            pltpu.VMEM((2, 4, 4, 16, 384), jnp.bfloat16),
            pltpu.VMEM((4, 4, 16, 128), jnp.bfloat16),
            pltpu.VMEM((2, 512, 768), jnp.bfloat16),
            pltpu.VMEM((4096, 128), F32),
            pltpu.VMEM((32, 8, 128), jnp.int32),
            pltpu.VMEM((32, 8, 128), jnp.int32),
            pltpu.VMEM((256, 128), jnp.int32),
            pltpu.VMEM((512, 8, 128), F32),
            pltpu.VMEM((512, 8, 128), F32),
            pltpu.VMEM((128, 4, 128), F32),
            pltpu.VMEM((512, 128), F32),
            pltpu.VMEM((512, 128), F32),
            pltpu.VMEM((128, 128), F32),
            pltpu.VMEM((128, 128), F32),
            pltpu.VMEM((64, 2, 128), F32),
            pltpu.VMEM((64, 2, 128), F32),
            dma((6,)), dma((1,)), dma((3,)), dma((3,)), dma((1,)), dma((5,)), dma((5,)), dma((5, 3)), dma((5,)),
            dma((5, 3)), dma((1,)), dma((1,)), dma((1,)), dma((1,)),
        ],
        compiler_params=pltpu.CompilerParams(collective_id=0, has_side_effects=True, vmem_limit_bytes=56550000),
    )(queries, probes, vectors, list_ids.reshape(4, 128), list_ids)


def solution(mesh):
    return jax.shard_map(
        local,
        mesh=mesh,
        in_specs=(
            P(("pb", "dev"), None),
            P(("pb", "dev"), None),
            P(("pb", "dev"), None),
            P(("pb", "dev")),
        ),
        out_specs=P(("pb", "dev"), None),
        check_vma=False,
    )
```
